32 devices in a mesh: seq: 8 (over z, x), expert: 4 (over y, core).
Axes of the slice: x: 2, y: 2, z: 4, core: 2. Of those that a mesh axis runs over, the one named last changes fastest.
Arguments:
- tokens: bfloat16 [1024, 4096], P('seq'), may hold values from -6 to 6
- norm_gain: float32 [4096], replicated, may hold values from 0.1 to 1.9
- router_weight: bfloat16 [4096, 4], replicated, may hold values from -0.09375 to 0.09375
- expert_ids: int32 [1024, 2], P('seq'), may hold values from 0 to 3, all different within a row; in each aligned block of 128 rows (0 to 127, 128 to 255, ...) at most 80 rows name the same one
- gate_weight: bfloat16 [4, 4096, 8192], P('expert', None, 'seq'), may hold values from -0.09375 to 0.09375
- up_weight: bfloat16 [4, 4096, 8192], P('expert', None, 'seq'), may hold values from -0.09375 to 0.09375
- down_weight: bfloat16 [4, 8192, 4096], P('expert', 'seq'), may hold values from -0.0625 to 0.0625
- query_weight: bfloat16 [4096, 2048], P(None, 'expert'), may hold values from -0.09375 to 0.09375
- key_weight: bfloat16 [4096, 2048], P(None, 'expert'), may hold values from -0.09375 to 0.09375
- log_decay: float32 [32, 1024], P('expert', 'seq'), may hold values from -1.5 to 0
- carried_state: float32 [32, 64, 128], P('expert'), may hold values from -48 to 48
- out_gain: float32 [4096], P('expert'), may hold values from 0.1 to 1.9
Outputs:
- teacher_out: bfloat16 [1024, 4096], P('seq', 'expert')
- student_out: bfloat16 [1024, 4096], P('seq', 'expert')
- token_loss: float32 [1024], P('seq')
The draws below stay inside these ranges and needn't reach their ends.
Inputs may be any that keep to these rules, and one draw needn't show every extreme that they name: `expert_ids`: each token names 2 different experts. Among the 128 tokens of one block no expert is named by more than 80 tokens, and in every draw some expert is named by exactly 80 tokens of some block.
All inputs are finite; a program needn't handle non-finite values.
Results may differ from the reference program's by a relative error of at most 0.01.
Values may be sent and summed in bfloat16 or wider, within the bound.
A program may use at most 128 MiB of HBM per device.

```python
import math
import jax
import jax.numpy as jnp
import numpy as np
from jax import lax

D = 4096
EXPERTS = 4
TOP = 2
FF = 8192
SPAN = 128
TOKEN_LENGTH = 1024
CAP = 56
LOAD = 80
HEAD = 128
KEY = 64
STUDENT_HEADS = 32
N_SEQ = 8


def draw_log_decay(key, part):
    key_sequence = jax.random.split(jax.random.fold_in(key, 17), 7)
    fast_share = 0.5
    blocks = TOKEN_LENGTH // SPAN
    fast_pick = jax.random.uniform(key_sequence[0], (STUDENT_HEADS, 1), jnp.float32) < fast_share
    fast_rate = jnp.exp(jax.random.uniform(key_sequence[1], (STUDENT_HEADS, 1), jnp.float32, jnp.log(1.0 / 50.0), jnp.log(1.0 / 30.0)))
    slow_rate = jnp.exp(jax.random.uniform(key_sequence[2], (STUDENT_HEADS, 1), jnp.float32, jnp.log(0.3), jnp.log(0.6))) / TOKEN_LENGTH
    base_rate = jnp.where(fast_pick, fast_rate, slow_rate)
    block_factor = jnp.exp(jax.random.uniform(key_sequence[3], (STUDENT_HEADS, blocks, 1), jnp.float32, jnp.log(0.7), jnp.log(1.5)))
    roughness = jax.random.uniform(key_sequence[4], (STUDENT_HEADS, blocks, SPAN), jnp.float32, 0.5, 1.5)
    decay_rates = (base_rate[:, :, None] * block_factor * roughness).reshape(STUDENT_HEADS, TOKEN_LENGTH)
    spike_position = jax.random.randint(key_sequence[5], (STUDENT_HEADS, 3, 1), 0, TOKEN_LENGTH)
    spike_loss = jax.random.uniform(key_sequence[6], (STUDENT_HEADS, 3, 1), jnp.float32, jnp.log(0.65), jnp.log(0.8))
    token_positions = jnp.arange(TOKEN_LENGTH)[None, None, :]
    spike_tokens = jnp.sum(jnp.where(token_positions == spike_position, spike_loss, 0.0), axis=1)
    return (spike_tokens - decay_rates).astype(jnp.float32)


def block_scale(key, extent, pieces, smallest, largest):
    level = 1.0
    for position, blocks in pieces:
        steps = jax.random.uniform(jax.random.fold_in(jax.random.fold_in(key, 6), position), (blocks,), jnp.float32, smallest / len(pieces), largest / len(pieces))
        level = level * jnp.repeat(jnp.exp(steps), extent[position] // blocks).reshape((-1,) + (1,) * (len(extent) - 1 - position))
    return level


def routed_block(rng, own, number, rows, count, top, bound, slope):
    order = jax.random.permutation(rng, count)
    crowded, common = load_shares(count, rows * top, bound, slope, True), load_shares(count, rows * top, bound, slope, False)
    places = jnp.arange(count)

    def named(lengths, offset_by):
        used = int((lengths > 0).sum())
        fixed = max(1, used // 4)
        passed = fixed + (places - fixed + offset_by * (used - fixed)) % max(1, count - fixed)
        return jnp.zeros((count,), jnp.int32).at[order[jnp.where(places < fixed, places, passed)]].set(jnp.asarray(lengths, jnp.int32))

    lengths = jnp.where(number % 4 == 0, named(crowded, number // 4), named(common, number - number // 4 - 1))
    mixed = jax.random.permutation(jax.random.fold_in(own, 3), count)
    source_of, sink = mixed[0:count // 2 * 2:2], mixed[1:count // 2 * 2:2]
    margin = jnp.minimum(lengths[source_of] - 1, bound - lengths[sink]) // 2
    margin = jnp.where((source_of == order[0]) | (sink == order[0]) | (lengths[sink] == 0), 0, jnp.maximum(margin, 0))
    passed = jax.random.randint(jax.random.fold_in(own, 4), (count // 2,), 0, 1 << 20) % (margin + 1)
    lengths = lengths.at[source_of].add(-passed).at[sink].add(passed)
    items = jnp.searchsorted(jnp.cumsum(lengths), jnp.arange(rows * top), side="right").astype(jnp.int32)
    listing = items.reshape(top, rows).T
    listing = listing[jax.random.permutation(jax.random.fold_in(own, 1), rows)]
    offset_by = jax.random.randint(jax.random.fold_in(own, 2), (rows, 1), 0, top)
    return jnp.take_along_axis(listing, (jnp.arange(top)[None, :] + offset_by) % top, axis=1)


def load_shares(count, total, limit, lean, full):
    loads = [(1 << 20) // math.isqrt(rank ** lean) + 1 for rank in range(1, count + 1)]
    largest = limit if full else min(limit, max(-(-total // count), total * loads[0] // sum(loads)))
    least = 1 if total - largest >= count - 1 else 0
    counts, spare = [largest] + [least] * (count - 1), total - largest - least * (count - 1)
    while spare > 0:
        candidates = [i for i in range(1, count) if counts[i] < largest] or [i for i in range(1, count) if counts[i] < limit]
        pool, budget = sum([loads[i] for i in candidates]), spare
        for i in candidates:
            extra = min(limit - counts[i], max(1, budget * loads[i] // pool), spare)
            counts[i] = counts[i] + extra
            spare = spare - extra
    return np.array(counts)


def noise(rng, shape, scale, limit, pieces=(), kind=jnp.bfloat16):
    result = scale * jax.random.normal(rng, shape, jnp.float32)
    if pieces:
        result = result * block_scale(rng, shape, pieces, -0.22, 0.18)
    return jnp.clip(result, -limit, limit).astype(kind)


def setup_inputs(seed: int = 0) -> dict:
    splits = jax.random.split(jax.random.key(seed), 13)
    tokens = noise(splits[0], (TOKEN_LENGTH, D), 1.0, 6.0, ((0, 8),))
    norm_gain = jnp.clip(1.0 + 0.18 * jax.random.normal(splits[1], (D,), jnp.float32), 0.1, 1.9)
    router_weight = noise(splits[2], (D, EXPERTS), D ** -0.5, 0.09375)
    expert_ids_keys = jax.random.split(jax.random.fold_in(splits[3], 1), TOKEN_LENGTH // SPAN)
    expert_ids_turns = jax.random.permutation(jax.random.fold_in(splits[3], 3), TOKEN_LENGTH // SPAN)
    expert_ids = jax.vmap(lambda own, number: routed_block(jax.random.fold_in(splits[3], 2), own, number, SPAN, EXPERTS, TOP, LOAD, 1))(expert_ids_keys, expert_ids_turns).reshape((TOKEN_LENGTH, TOP))
    gate_weight = noise(splits[4], (EXPERTS, D, FF), D ** -0.5, 0.09375, ((0, 4), (2, 8)))
    up_weight = noise(splits[5], (EXPERTS, D, FF), D ** -0.5, 0.09375, ((0, 4), (2, 8)))
    down_weight = noise(splits[6], (EXPERTS, FF, D), FF ** -0.5, 0.0625, ((0, 4), (1, 8)))
    query_weight = noise(splits[7], (D, STUDENT_HEADS * KEY), D ** -0.5, 0.09375, ((1, 4),))
    key_weight = noise(splits[8], (D, STUDENT_HEADS * KEY), D ** -0.5, 0.09375, ((1, 4),))
    log_decay = draw_log_decay(jax.random.fold_in(splits[12], 71), 0)
    carried_state = noise(splits[10], (STUDENT_HEADS, KEY, HEAD), 8.0, 48.0, ((0, 4),), jnp.float32)
    out_gain = jnp.clip(1.0 + 0.18 * jax.random.normal(splits[11], (D,), jnp.float32), 0.1, 1.9)
    return {"tokens": tokens, "norm_gain": norm_gain, "router_weight": router_weight, "expert_ids": expert_ids, "gate_weight": gate_weight, "up_weight": up_weight, "down_weight": down_weight, "query_weight": query_weight, "key_weight": key_weight, "log_decay": log_decay, "carried_state": carried_state, "out_gain": out_gain}


norm_epsilon = 1e-05
head_epsilon = 1e-06
peak_error = lax.Precision.HIGHEST

def reference(tokens, norm_gain, router_weight, expert_ids, gate_weight, up_weight, down_weight, query_weight, key_weight, log_decay, carried_state, out_gain):
    tok_float = tokens.astype(jnp.float32)
    normed = (tok_float * lax.rsqrt(lax.optimization_barrier(jnp.mean(tok_float * tok_float, axis=1, keepdims=True)) + norm_epsilon) * norm_gain).astype(jnp.bfloat16)
    logits = jnp.dot(normed, router_weight, preferred_element_type=jnp.float32)
    expert_iota = jnp.arange(EXPERTS, dtype=jnp.int32)
    picks = expert_ids[:, :, None] == expert_iota[None, None, :]
    chosen = lax.optimization_barrier(jnp.sum(jnp.where(picks, logits[:, None, :], jnp.float32(0.0)), axis=2))
    first_share = 1.0 / (1.0 + jnp.exp(chosen[:, 1] - chosen[:, 0]))
    shares = jnp.stack([first_share, 1.0 - first_share], axis=1)
    mix_weight = lax.optimization_barrier(jnp.sum(jnp.where(picks, shares[:, :, None], jnp.float32(0.0)), axis=1))
    hits = jnp.any(picks, axis=1).astype(jnp.int32)
    blocks = TOKEN_LENGTH // SPAN
    block_hits = hits.reshape(blocks, SPAN, EXPERTS)
    block_slots = jnp.cumsum(block_hits, axis=1) - block_hits
    block_weight = mix_weight.reshape(blocks, SPAN, EXPERTS)
    slot_iota = jnp.arange(CAP, dtype=jnp.int32)
    normed_blocks = normed.reshape(blocks, SPAN, D).astype(jnp.float32)
    ff_part = FF // N_SEQ

    def one_expert(mixed, inputs):
        expert_index, gate_mat, up_mat, down_mat = inputs
        chosen_col = expert_iota[None, None, :] == expert_index
        own_hits = lax.optimization_barrier(jnp.sum(jnp.where(chosen_col, block_hits, 0), axis=2))
        own_slots = lax.optimization_barrier(jnp.sum(jnp.where(chosen_col, block_slots, 0), axis=2))
        own_weight = lax.optimization_barrier(jnp.sum(jnp.where(chosen_col, block_weight, jnp.float32(0.0)), axis=2))
        select = ((own_hits[:, None, :] == 1) & (own_slots[:, None, :] == slot_iota[None, :, None])).astype(jnp.float32)
        rows = jnp.einsum('cpt,ctd->cpd', select, normed_blocks, precision=peak_error).astype(jnp.bfloat16).reshape(blocks * CAP, D)
        gate_proj = jnp.dot(rows, gate_mat, preferred_element_type=jnp.float32)
        up_proj = jnp.dot(rows, up_mat, preferred_element_type=jnp.float32)
        hidden = (jax.nn.silu(gate_proj) * up_proj).astype(jnp.bfloat16)

        def add_part(total, part_index):
            hidden_part = lax.dynamic_slice_in_dim(hidden, part_index * ff_part, ff_part, 1)
            down_part = lax.dynamic_slice_in_dim(down_mat, part_index * ff_part, ff_part, 0)
            partial_value = jnp.dot(hidden_part, down_part, preferred_element_type=jnp.float32).astype(jnp.bfloat16)
            partial_value = lax.optimization_barrier(partial_value)
            return (total + partial_value.astype(jnp.float32), None)
        total, _ = lax.scan(add_part, jnp.zeros((blocks * CAP, D), jnp.float32), jnp.arange(N_SEQ, dtype=jnp.int32))
        rounded = lax.optimization_barrier(total.astype(jnp.bfloat16))
        expert_rows = rounded.astype(jnp.float32).reshape(blocks, CAP, D)
        weigh = select * own_weight[:, None, :]
        spread = jnp.einsum('cpt,cpd->ctd', weigh, expert_rows, precision=peak_error).reshape(TOKEN_LENGTH, D)
        return (mixed + spread, None)
    mixed, _ = lax.scan(one_expert, jnp.zeros((TOKEN_LENGTH, D), jnp.float32), (expert_iota, gate_weight, up_weight, down_weight))
    teacher_hidden = tok_float + mixed

    def to_blocks(matrix, features):
        return matrix.reshape(TOKEN_LENGTH, STUDENT_HEADS, features).transpose(1, 0, 2).reshape(STUDENT_HEADS, blocks, SPAN, features).transpose(1, 0, 2, 3)
    query_rows = to_blocks(jnp.dot(tokens, query_weight, preferred_element_type=jnp.float32), KEY)
    keys_proj = to_blocks(jnp.dot(tokens, key_weight, preferred_element_type=jnp.float32), KEY)
    value_rows = to_blocks(tok_float, HEAD)
    decays = log_decay.reshape(STUDENT_HEADS, blocks, SPAN).transpose(1, 0, 2)
    lower = jnp.arange(SPAN)[:, None] >= jnp.arange(SPAN)[None, :]

    def one_block(recurrent_state, inputs):
        query_block, block_k, value_block, block_g = inputs
        running_state = jnp.cumsum(block_g, axis=1)
        last_state = running_state[:, -1]
        gaps = running_state[:, :, None] - running_state[:, None, :]
        weights = jnp.where(lower[None], jnp.exp(jnp.minimum(gaps, 0.0)), 0.0)
        scores = jnp.einsum('htk,hsk->hts', query_block, block_k, precision=peak_error) * weights
        output_rows = jnp.einsum('hts,hsv->htv', scores, value_block, precision=peak_error)
        output_rows = output_rows + jnp.exp(running_state)[:, :, None] * jnp.einsum('ezy,eyl->ezl', query_block, recurrent_state, precision=peak_error)
        scaled_keys = block_k * jnp.exp(last_state[:, None] - running_state)[:, :, None]
        recurrent_state = jnp.exp(last_state)[:, None, None] * recurrent_state + jnp.einsum('wpl,wpg->wlg', scaled_keys, value_block, precision=peak_error)
        return (recurrent_state, output_rows)
    _, output_rows = lax.scan(one_block, carried_state.astype(jnp.float32), (query_rows, keys_proj, value_rows, decays))
    normed_out = output_rows * lax.rsqrt(lax.optimization_barrier(jnp.mean(output_rows * output_rows, axis=3, keepdims=True)) + head_epsilon)
    branch = normed_out.transpose(0, 2, 1, 3).reshape(TOKEN_LENGTH, D) * out_gain
    student_hidden = tok_float + branch
    gap = student_hidden - teacher_hidden
    token_loss = lax.optimization_barrier(jnp.mean(gap * gap, axis=1))
    return (teacher_hidden.astype(jnp.bfloat16), student_hidden.astype(jnp.bfloat16), token_loss)
```

```python
import functools
import jax
import jax.numpy as jnp
from jax import lax
from jax.experimental import pallas as pl
from jax.experimental.pallas import tpu as pltpu
from jax.sharding import PartitionSpec as P

norm_epsilon = 1e-05
head_epsilon = 1e-06
exact = lax.Precision.HIGHEST
f32 = jnp.float32
bf16 = jnp.bfloat16
LANES = 128
SUB = 8
MESH = pl.DeviceIdType.MESH


def ring_order(mesh):
    n = mesh.shape["seq"]
    line = mesh.devices[:, 0]
    coords = [getattr(d, "coords", None) for d in line]
    if any(c is None for c in coords):
        return list(range(n))
    places = {(c[0], c[2]): i for i, c in enumerate(coords)}
    xs = sorted({x for x, _ in places})
    zs = sorted({z for _, z in places})
    if len(places) != n or len(xs) * len(zs) != n or len(xs) % 2 or len(zs) < 2:
        return list(range(n))
    order = [places[(x, zs[0])] for x in xs]
    for turn, x in enumerate(reversed(xs)):
        column = zs[1:] if turn % 2 == 0 else zs[:0:-1]
        order += [places[(x, z)] for z in column]
    return order


def split(value):
    high = value.astype(bf16)
    low = (value - high.astype(f32)).astype(bf16)
    return high, low


def dot(a, b, dims=(1, 0), precision=None):
    return lax.dot_general(
        a,
        b,
        (((dims[0],), (dims[1],)), ((), ())),
        preferred_element_type=f32,
        precision=precision,
    )


def layer_kernel(
    order,
    cap,
    tok_hbm,
    gain,
    router,
    ids,
    gate_hbm,
    up_hbm,
    down_hbm,
    query_hbm,
    key_hbm,
    decay,
    carried,
    out_gain,
    teacher_out,
    student_out,
    loss_out,
    tok,
    gate,
    up,
    down,
    wq,
    wk,
    normed,
    rows,
    part,
    inbox,
    lhs,
    hid,
    qs,
    ks,
    run_s,
    run_t,
    retain_own,
    block_state,
    prior,
    pair_out,
    pair_in,
    retain_in,
    chain_out,
    chain_in,
    mix_high,
    mix_low,
    intra,
    expert_out,
    expert_in,
    loss_all,
    load_sem,
    ag_send,
    ag_recv,
    rs_send,
    rs_recv,
    st_send,
    st_recv,
    ex_send,
    ex_recv,
    lo_send,
    lo_recv,
):
    n = len(order)
    half = n // 2
    span, width = tok.shape
    half_cols = width // 2
    ff = gate.shape[1]
    groups = lax.axis_size("expert")
    bw = width // groups
    g = rows.shape[2]
    capp = g * SUB
    heads = decay.shape[0]
    key_size = block_state.shape[0] // heads
    per = LANES // key_size
    place = lax.axis_index("seq")
    mine = lax.axis_index("expert")
    pairs = n // 2
    pair = place // 2
    odd = place % 2

    def table(values):
        found = jnp.int32(0)
        for i, v in enumerate(values):
            found = jnp.where(place == i, jnp.int32(v), found)
        return found

    at = {s: k for k, s in enumerate(order)}
    right = table([order[(at[i] + 1) % n] for i in range(n)])
    left = table([order[(at[i] - 1) % n] for i in range(n)])
    sides = (right, left)
    partner = place + 1 - 2 * odd
    ahead = lax.rem(place + 2, n)
    behind = lax.rem(place + n - 2, n)

    loads = []
    for i, (src, dst) in enumerate(
        ((tok_hbm, tok), (key_hbm, wk), (query_hbm, wq), (gate_hbm, gate), (up_hbm, up), (down_hbm, down))
    ):
        copy = pltpu.make_async_copy(src, dst, load_sem.at[i])
        copy.start()
        loads.append(copy)

    barrier = pltpu.get_barrier_semaphore()
    for there in (right, left, partner, ahead, behind):
        pl.semaphore_signal(barrier, inc=1, device_id={"seq": there}, device_id_type=MESH)
    for shift in range(1, groups):
        peer = lax.rem(mine + shift, groups)
        pl.semaphore_signal(barrier, inc=1, device_id={"expert": peer}, device_id_type=MESH)

    sent = []

    def send(src, dst, send_sem, recv_sem, **to):
        copy = pltpu.make_async_remote_copy(
            src_ref=src,
            dst_ref=dst,
            send_sem=send_sem,
            recv_sem=recv_sem,
            device_id=to,
            device_id_type=MESH,
        )
        copy.start()
        return copy

    def arrived(dst, sem):
        pltpu.make_async_copy(dst, dst, sem).wait()

    loads[0].wait()
    strip = 16

    def norm_strip(i, _):
        at_rows = pl.ds(pl.multiple_of(i * strip, strip), strip)
        x = tok[at_rows, :].astype(f32)
        scale = lax.rsqrt(jnp.mean(x * x, axis=1, keepdims=True) + norm_epsilon)
        normed[at_rows, :] = (x * scale * gain[...]).astype(bf16)
        return 0

    lax.fori_loop(0, span // strip, norm_strip, 0)
    experts = router.shape[1]
    logits = dot(normed[...], router[...])
    id0 = ids[:, 0:1]
    id1 = ids[:, 1:2]
    lane_e = lax.broadcasted_iota(jnp.int32, (span, experts), 1)
    chosen0 = jnp.sum(jnp.where(lane_e == id0, logits, 0.0), axis=1, keepdims=True)
    chosen1 = jnp.sum(jnp.where(lane_e == id1, logits, 0.0), axis=1, keepdims=True)
    share0 = 1.0 / (1.0 + jnp.exp(chosen1 - chosen0))
    share1 = 1.0 - share0
    row_t = lax.broadcasted_iota(jnp.int32, (span, span), 0)
    col_t = lax.broadcasted_iota(jnp.int32, (span, span), 1)
    lane = lax.broadcasted_iota(jnp.int32, (span, LANES), 1)
    hits = jnp.where((lane == id0) | (lane == id1), 1.0, 0.0).astype(bf16)
    before = jnp.where(row_t > col_t, 1.0, 0.0).astype(bf16)
    slots = dot(before, hits)
    own_lane = jnp.where(
        lax.broadcasted_iota(jnp.int32, (SUB, LANES), 1) == mine, 1.0, 0.0
    ).astype(bf16)
    hit_row = dot(own_lane, hits, (1, 1))
    slot_row = dot(own_lane, slots.astype(bf16), (1, 1))
    want = lax.broadcasted_iota(jnp.int32, (capp, span), 0)
    picked = (slot_row[0:1, :].astype(jnp.int32) == want) & (hit_row[0:1, :] > 0.5) & (want < cap)
    select = jnp.where(picked, 1.0, 0.0).astype(bf16)
    step_cols = 512
    for h in range(2):

        def dispatch(i, _, h=h):
            off = pl.multiple_of(i * step_cols, step_cols)
            got = dot(select, normed[:, pl.ds(h * half_cols + off, step_cols)])
            rows[0, h, :, :, pl.ds(off, step_cols)] = got.reshape(g, SUB, step_cols).astype(bf16)
            return 0

        lax.fori_loop(0, half_cols // step_cols, dispatch, 0)

    pl.semaphore_wait(barrier, 5 + groups - 1)

    def spot(rel):
        return rel % n

    def ag_step(k, side, h):
        sign = -1 if side == 0 else 1
        src = spot(sign * (k - 1))
        dst = spot(sign * k)
        sent.append(
            send(
                rows.at[src, h],
                rows.at[dst, h],
                ag_send.at[side, k, h],
                ag_recv.at[side, k, h],
                seq=sides[side],
            )
        )

    for ci in range(2):
        for side in range(2):
            ag_step(1, side, ci if side == 0 else 1 - ci)

    def ag_event(k, ci):
        for side in range(2):
            h = ci if side == 0 else 1 - ci
            sign = -1 if side == 0 else 1
            arrived(rows.at[spot(sign * k), h], ag_recv.at[side, k, h])
            if k + 1 < half or (k + 1 == half and ci == 0):
                ag_step(k + 1, side, h)

    wide = groups * capp
    lane_w = lax.broadcasted_iota(jnp.int32, (span, wide), 1)
    mixing = jnp.zeros((span, wide), f32)
    for shift in range(groups):
        source = lax.rem(mine + groups - shift, groups)
        slot = jnp.sum(jnp.where(lane == source, slots, 0.0), axis=1, keepdims=True).astype(jnp.int32)
        first, second = id0 == source, id1 == source
        share = jnp.where(first, share0, jnp.where(second, share1, 0.0))
        share = jnp.where(slot < cap, share, 0.0)
        mixing = mixing + jnp.where(lane_w == slot + shift * capp, share, 0.0)
    high, low = split(mixing)
    mix_high[...] = high
    mix_low[...] = low

    loads[1].wait()
    ks[...] = dot(tok[...], wk[...])
    loads[2].wait()
    qs[...] = dot(tok[...], wq[...])

    lower = row_t >= col_t
    tri = jnp.where(lower, 1.0, 0.0)
    run_s[...] = dot(decay[...], tri, (1, 1), exact)
    run_t[...] = dot(tri, decay[...], (1, 1), exact)
    retain_own[...] = jnp.exp(jnp.broadcast_to(run_s[:, span - 1 : span], (heads, LANES)))

    def values_of(head):
        return tok[:, pl.ds(pl.multiple_of(mine * bw + head * LANES, LANES), LANES)]

    def state_unit(p):
        tail = jnp.exp(run_t[span - 1 : span, :] - run_t[...])
        factor = jnp.zeros((span, LANES), f32)
        for a in range(per):
            inside = (lane >= a * key_size) & (lane < (a + 1) * key_size)
            factor = jnp.where(inside, tail[:, p * per + a : p * per + a + 1], factor)
        scaled = (ks[:, p * LANES : (p + 1) * LANES] * factor).T
        hi, lo = split(scaled)
        for a in range(per):
            head = p * per + a
            values = values_of(head)
            cut = slice(a * key_size, (a + 1) * key_size)
            block_state[head * key_size : (head + 1) * key_size, :] = (
                dot(hi, values) + dot(lo, values)
            )[cut]

    for p in range(heads // per):
        state_unit(p)
    pair_out[...] = block_state[...].astype(bf16)
    state_sent = [
        send(pair_out, pair_in, st_send.at[0], st_recv.at[0], seq=partner),
        send(retain_own, retain_in, st_send.at[1], st_recv.at[1], seq=partner),
    ]

    def chain_point(j):
        if j == 0:
            arrived(pair_in, st_recv.at[0])
            arrived(retain_in, st_recv.at[1])

        @pl.when(pair == j)
        def _():
            if j > 0:
                arrived(chain_in, st_recv.at[2])
            for head in range(heads):
                at_head = slice(head * key_size, (head + 1) * key_size)
                coming = carried[at_head, :] if j == 0 else chain_in[at_head, :].astype(f32)
                own_keep = retain_own[head : head + 1, :]
                other_keep = retain_in[head : head + 1, :]
                own = block_state[at_head, :]
                other = pair_in[at_head, :].astype(f32)
                is_odd = odd == 1
                prior[at_head, :] = jnp.where(is_odd, other_keep * coming + other, coming)
                if j < pairs - 1:
                    both = jnp.where(is_odd, own_keep * other + own, other_keep * own + other)
                    chain_out[at_head, :] = (own_keep * other_keep * coming + both).astype(bf16)
            if j < pairs - 1:
                send(chain_out, chain_in, st_send.at[2], st_recv.at[2], seq=ahead)

    batches = [[0]] + [[k, -k] for k in range(1, half)] + [[half]]

    def gate_up(b):
        members = batches[b]
        m = len(members) * capp

        def gather(i, _):
            off = pl.multiple_of(i * step_cols, step_cols)
            for h in range(2):
                got = [
                    rows[spot(rel), h, :, :, pl.ds(off, step_cols)].astype(f32).reshape(capp, step_cols)
                    for rel in members
                ]
                got = jnp.concatenate(got, axis=0) if len(got) > 1 else got[0]
                lhs[0:m, pl.ds(h * half_cols + off, step_cols)] = got.astype(bf16)
            return 0

        lax.fori_loop(0, half_cols // step_cols, gather, 0)
        tile = min(256, ff)

        def columns(i, _):
            cols = pl.ds(pl.multiple_of(i * tile, tile), tile)
            a = lhs[0:m, :]
            gated = dot(a, gate[:, cols])
            upped = dot(a, up[:, cols])
            silu = gated / (1.0 + jnp.exp(-gated))
            hid[b, 0:m, cols] = (silu * upped).astype(bf16)
            return 0

        lax.fori_loop(0, ff // tile, columns, 0)

    def down_proj(b, h):
        members = batches[b]
        m = len(members) * capp

        def columns(i, _):
            off = pl.multiple_of(i * step_cols, step_cols)
            got = dot(hid[b, 0:m, :], down[:, pl.ds(h * half_cols + off, step_cols)])
            for j, rel in enumerate(members):
                piece = got[j * capp : (j + 1) * capp].reshape(g, SUB, step_cols)
                part[spot(rel), h, :, :, pl.ds(off, step_cols)] = piece.astype(bf16)
            return 0

        lax.fori_loop(0, half_cols // step_cols, columns, 0)

    def rs_step(k, side, h, add):
        rel = spot(k if side == 0 else -k)
        if add:
            arrived(inbox.at[side, k + 1, h], rs_recv.at[side, k + 1, h])

            def add_cols(i, _):
                cols = pl.ds(pl.multiple_of(i * step_cols, step_cols), step_cols)
                total = part[rel, h, :, :, cols].astype(f32) + inbox[side, k + 1, h, :, :, cols].astype(f32)
                part[rel, h, :, :, cols] = total.astype(bf16)
                return 0

            lax.fori_loop(0, half_cols // step_cols, add_cols, 0)
        sent.append(
            send(
                part.at[rel, h],
                inbox.at[side, k, h],
                rs_send.at[side, k, h],
                rs_recv.at[side, k, h],
                seq=sides[side],
            )
        )

    def free_chain(k, add):
        for side in range(2):
            rs_step(k, side, 1 - side, add)

    def far_chain(k, add):
        for side in range(2):
            rs_step(k, side, side, add)

    def intra_unit(p):
        q_pair = qs[:, p * LANES : (p + 1) * LANES]
        k_hi, k_lo = split(ks[:, p * LANES : (p + 1) * LANES])
        for a in range(per):
            head = p * per + a
            inside = (lane >= a * key_size) & (lane < (a + 1) * key_size)
            q_hi, q_lo = split(jnp.where(inside, q_pair, 0.0))
            scores = dot(q_hi, k_hi, (1, 1)) + dot(q_hi, k_lo, (1, 1)) + dot(q_lo, k_hi, (1, 1))
            gaps = run_t[:, head : head + 1] - run_s[head : head + 1, :]
            scores = scores * jnp.where(row_t >= col_t, jnp.exp(jnp.minimum(gaps, 0.0)), 0.0)
            s_hi, s_lo = split(scores)
            values = values_of(head)
            intra[:, head * LANES : (head + 1) * LANES] = dot(s_hi, values) + dot(s_lo, values)

    def inter_unit(p):
        q_pair = qs[:, p * LANES : (p + 1) * LANES]
        s_hi, s_lo = split(prior[p * LANES : (p + 1) * LANES, :])
        for a in range(per):
            head = p * per + a
            cols = slice(head * LANES, (head + 1) * LANES)
            inside = (lane >= a * key_size) & (lane < (a + 1) * key_size)
            q_hi, q_lo = split(jnp.where(inside, q_pair, 0.0))
            carried_rows = dot(q_hi, s_hi) + dot(q_hi, s_lo) + dot(q_lo, s_hi)
            out = intra[:, cols] + jnp.exp(run_t[:, head : head + 1]) * carried_rows
            scale = lax.rsqrt(jnp.mean(out * out, axis=1, keepdims=True) + head_epsilon)
            hidden = values_of(head).astype(f32) + out * scale * out_gain[:, cols]
            intra[:, cols] = hidden
            student_out[:, cols] = hidden.astype(bf16)

    loads[3].wait()
    loads[4].wait()
    for k in range(1, half):
        ag_event(k, 0)
        if k == 1:
            gate_up(0)
        if k == 2:
            chain_point(0)
            for p in range(heads // per):
                intra_unit(p)
        ag_event(k, 1)
        gate_up(k)
    loads[5].wait()
    down_proj(half - 1, 0)
    down_proj(half - 1, 1)
    free_chain(half - 1, False)
    ag_event(half, 0)
    gate_up(half)
    down_proj(half, 0)
    down_proj(half, 1)
    far_chain(half, False)
    link = 1
    for k in range(half - 1, 0, -1):
        if link < pairs:
            chain_point(link)
            link += 1
        for h in range(2):
            down_proj(k - 1, h)
        if k > 1:
            free_chain(k - 1, True)
        else:
            for p in range(heads // per):
                inter_unit(p)
        far_chain(k, True)

    for side in range(2):
        for h in range(2):
            arrived(inbox.at[side, 1, h], rs_recv.at[side, 1, h])
    per_half = groups // 2
    for q in range(groups):
        h = q // per_half
        cols = pl.ds((q % per_half) * bw, bw)
        total = part[0, h, :, :, cols].astype(f32)
        total = total + inbox[0, 1, h, :, :, cols].astype(f32) + inbox[1, 1, h, :, :, cols].astype(f32)
        expert_out[q] = total.astype(bf16)
    for shift in [groups // 2] + [i for i in range(1, groups) if i != groups // 2]:
        peer = lax.rem(mine + shift, groups)
        sent.append(
            send(
                expert_out.at[peer], expert_in.at[shift], ex_send.at[shift], ex_recv.at[shift], expert=peer
            )
        )
    expert_in[0] = expert_out[mine]
    for shift in range(1, groups):
        arrived(expert_in.at[shift], ex_recv.at[shift])
    loss_row = jnp.zeros((SUB, span), f32)
    ones = jnp.ones((SUB, step_cols), f32)
    for i in range(bw // step_cols):
        cols = slice(i * step_cols, (i + 1) * step_cols)
        got = [expert_in[shift, :, :, cols].astype(f32).reshape(capp, step_cols) for shift in range(groups)]
        got = jnp.concatenate(got, axis=0).astype(bf16)
        mixed = dot(mix_high[...], got) + dot(mix_low[...], got)
        own = tok[:, pl.ds(pl.multiple_of(mine * bw + i * step_cols, LANES), step_cols)].astype(f32)
        hidden = own + mixed
        teacher_out[:, cols] = hidden.astype(bf16)
        gap = intra[:, cols] - hidden
        loss_row = loss_row + dot(ones, gap * gap, (1, 1), exact)
    loss_all[mine] = loss_row
    for shift in range(1, groups):
        peer = lax.rem(mine + shift, groups)
        sent.append(
            send(loss_all.at[mine], loss_all.at[mine], lo_send.at[shift], lo_recv.at[mine], expert=peer)
        )
    for shift in range(1, groups):
        peer = lax.rem(mine + shift, groups)
        arrived(loss_all.at[peer], lo_recv.at[peer])
    total = loss_all[0]
    for q in range(1, groups):
        total = total + loss_all[q]
    loss_out[...] = total / width

    for copy in sent + state_sent:
        copy.wait_send()

    @pl.when(pair < pairs - 1)
    def _():
        pltpu.make_async_copy(chain_out, chain_out, st_send.at[2]).wait()


def on_device(
    order,
    tokens,
    norm_gain,
    router_weight,
    expert_ids,
    gate_weight,
    up_weight,
    down_weight,
    query_weight,
    key_weight,
    log_decay,
    carried_state,
    out_gain,
):
    span, width = tokens.shape
    experts = router_weight.shape[1]
    groups = lax.axis_size("expert")
    cap = 7 * expert_ids.shape[1] * span // (8 * experts)
    g = -(-cap // SUB)
    capp = g * SUB
    n = len(order)
    half = n // 2
    half_cols = width // 2
    ff = gate_weight.shape[2]
    bw = width // groups
    heads, key_size, feats = carried_state.shape
    keys = heads * key_size
    hbm = pl.BlockSpec(memory_space=pl.ANY)
    vmem = pl.BlockSpec(memory_space=pltpu.VMEM)
    dma = pltpu.SemaphoreType.DMA
    scratch = [
        pltpu.VMEM((span, width), bf16),
        pltpu.VMEM((width, ff), bf16),
        pltpu.VMEM((width, ff), bf16),
        pltpu.VMEM((ff, width), bf16),
        pltpu.VMEM((width, keys), bf16),
        pltpu.VMEM((width, keys), bf16),
        pltpu.VMEM((span, width), bf16),
        pltpu.VMEM((n, 2, g, SUB, half_cols), bf16),
        pltpu.VMEM((n, 2, g, SUB, half_cols), bf16),
        pltpu.VMEM((2, half + 1, 2, g, SUB, half_cols), bf16),
        pltpu.VMEM((2 * capp, width), bf16),
        pltpu.VMEM((half + 1, 2 * capp, ff), bf16),
        pltpu.VMEM((span, keys), f32),
        pltpu.VMEM((span, keys), f32),
        pltpu.VMEM((heads, span), f32),
        pltpu.VMEM((span, heads), f32),
        pltpu.VMEM((heads, LANES), f32),
        pltpu.VMEM((keys, feats), f32),
        pltpu.VMEM((keys, feats), f32),
        pltpu.VMEM((keys, feats), bf16),
        pltpu.VMEM((keys, feats), bf16),
        pltpu.VMEM((heads, LANES), f32),
        pltpu.VMEM((keys, feats), bf16),
        pltpu.VMEM((keys, feats), bf16),
        pltpu.VMEM((span, groups * capp), bf16),
        pltpu.VMEM((span, groups * capp), bf16),
        pltpu.VMEM((span, bw), f32),
        pltpu.VMEM((groups, g, SUB, bw), bf16),
        pltpu.VMEM((groups, g, SUB, bw), bf16),
        pltpu.VMEM((groups, SUB, span), f32),
        dma((6,)),
        dma((2, half + 1, 2)),
        dma((2, half + 1, 2)),
        dma((2, half + 1, 2)),
        dma((2, half + 1, 2)),
        dma((3,)),
        dma((3,)),
        dma((groups,)),
        dma((groups,)),
        dma((groups,)),
        dma((groups,)),
    ]
    teacher, student, loss = pl.pallas_call(
        functools.partial(layer_kernel, order, cap),
        out_shape=(
            jax.ShapeDtypeStruct((span, bw), bf16),
            jax.ShapeDtypeStruct((span, bw), bf16),
            jax.ShapeDtypeStruct((SUB, span), f32),
        ),
        in_specs=[hbm, vmem, vmem, vmem, hbm, hbm, hbm, hbm, hbm, vmem, vmem, vmem],
        out_specs=(vmem, vmem, vmem),
        scratch_shapes=scratch,
        compiler_params=pltpu.CompilerParams(
            collective_id=0, has_side_effects=True, vmem_limit_bytes=62 * 1024 * 1024
        ),
        name="layer",
    )(
        tokens,
        norm_gain.reshape(1, width),
        router_weight,
        expert_ids,
        gate_weight.reshape(width, ff),
        up_weight.reshape(width, ff),
        down_weight.reshape(ff, width),
        query_weight,
        key_weight,
        log_decay,
        carried_state.reshape(keys, feats),
        out_gain.reshape(1, bw),
    )
    return teacher, student, loss[0]


def solution(mesh):
    return jax.shard_map(
        functools.partial(on_device, tuple(ring_order(mesh))),
        mesh=mesh,
        in_specs=(
            P("seq", None),
            P(),
            P(),
            P("seq", None),
            P("expert", None, "seq"),
            P("expert", None, "seq"),
            P("expert", "seq", None),
            P(None, "expert"),
            P(None, "expert"),
            P("expert", "seq"),
            P("expert", None, None),
            P("expert"),
        ),
        out_specs=(P("seq", "expert"), P("seq", "expert"), P("seq")),
        check_vma=False,
    )
```

```python
import functools
import jax
import jax.numpy as jnp
from jax import lax
from jax.experimental import pallas as pl
from jax.experimental.pallas import tpu as pltpu
from jax.sharding import PartitionSpec as P

norm_epsilon = 1e-05
head_epsilon = 1e-06
exact = lax.Precision.HIGHEST
f32 = jnp.float32
bf16 = jnp.bfloat16
LANES = 128
SUB = 8
MESH = pl.DeviceIdType.MESH


def ring_order(mesh):
    n = mesh.shape["seq"]
    line = mesh.devices[:, 0]
    coords = [getattr(d, "coords", None) for d in line]
    if any(c is None for c in coords):
        return list(range(n))
    places = {(c[0], c[2]): i for i, c in enumerate(coords)}
    xs = sorted({x for x, _ in places})
    zs = sorted({z for _, z in places})
    if len(places) != n or len(xs) * len(zs) != n or len(xs) % 2 or len(zs) < 2:
        return list(range(n))
    order = [places[(x, zs[0])] for x in xs]
    for turn, x in enumerate(reversed(xs)):
        column = zs[1:] if turn % 2 == 0 else zs[:0:-1]
        order += [places[(x, z)] for z in column]
    return order


def split(value):
    high = value.astype(bf16)
    low = (value - high.astype(f32)).astype(bf16)
    return high, low


def dot(a, b, dims=(1, 0), precision=None):
    return lax.dot_general(
        a,
        b,
        (((dims[0],), (dims[1],)), ((), ())),
        preferred_element_type=f32,
        precision=precision,
    )


class Plan:
    link_rate = 45000.0
    latency = 2.8

    def __init__(self):
        self.now = 0.0
        self.free = 0.0
        self.arrival = {}
        self.units = []
        self.done = set()

    def unit(self, name, cost, work, after=(), messages=(), start=0.0):
        self.units.append((name, cost, work, tuple(after), tuple(messages), start))

    def ready(self, unit):
        name, cost, work, after, messages, start = unit
        if any(a not in self.done for a in after) or any(m not in self.arrival for m in messages):
            return None
        return max([start] + [self.arrival[m] + 1.0 for m in messages])

    def run(self, unit):
        name, cost, work, after, messages, start = unit
        self.units.remove(unit)
        for a in after:
            self.force(a)
        self.now = max([self.now] + [self.arrival[m] for m in messages])
        work()
        self.now += cost
        self.done.add(name)

    def force(self, name):
        for unit in self.units:
            if unit[0] == name:
                self.run(unit)
                return
        assert name in self.done

    def fill(self, until):
        while True:
            for unit in self.units:
                when = self.ready(unit)
                if when is not None and when <= self.now and self.now + unit[1] <= until:
                    self.run(unit)
                    break
            else:
                later = [self.ready(u) for u in self.units]
                later = [w for w in later if w is not None and self.now < w < until]
                if not later:
                    return
                self.now = min(later)

    def message(self, name, size, work, before=None, needs=()):
        for a in needs:
            self.force(a)
        ready = self.arrival[before] if before is not None else self.now
        self.fill(max(ready, self.free - 0.5))
        self.now = max(self.now, ready)
        work()
        self.now += 0.1
        self.free = max(self.free, self.now) + size / self.link_rate
        self.arrival[name] = self.free + self.latency

    def drain(self):
        while self.units:
            known = [(self.ready(u), i) for i, u in enumerate(self.units)]
            known = [w for w in known if w[0] is not None]
            self.run(self.units[min(known)[1]])


def layer_kernel(
    order,
    cap,
    parts,
    cuts,
    tok_hbm,
    gain_hbm,
    router_hbm,
    ids_hbm,
    gate_hbm,
    up_hbm,
    down_hbm,
    query_hbm,
    key_hbm,
    decay_hbm,
    carried_hbm,
    out_gain_hbm,
    teacher_hbm,
    student_hbm,
    loss_out,
    gain,
    router,
    ids,
    decay,
    carried,
    out_gain,
    teacher_out,
    student_out,
    tok,
    gate,
    up,
    down,
    wq,
    wk,
    normed,
    lhs,
    qs,
    ks,
    run_s,
    run_t,
    retain_own,
    block_state,
    prior,
    pair_out,
    pair_in,
    retain_in,
    chain_out,
    chain_in,
    intra,
    teacher,
    slot_s,
    loss_all,
    rows,
    part,
    inbox,
    hid,
    mix_high,
    mix_low,
    expert_out,
    expert_in,
    load_sem,
    ag_send,
    ag_recv,
    rs_send,
    rs_recv,
    st_send,
    st_recv,
    ex_send,
    ex_recv,
    lo_send,
    lo_recv,
):
    n = len(order)
    half = n // 2
    span, width = tok.shape
    cut_cols = width // cuts
    ff = gate.shape[1]
    groups = lax.axis_size("expert")
    bw = width // groups
    capp = sum(parts) * SUB
    heads = decay.shape[0]
    key_size = block_state.shape[0] // heads
    per = LANES // key_size
    place = lax.axis_index("seq")
    mine = lax.axis_index("expert")
    pairs = n // 2
    pair = place // 2
    odd = place % 2
    step_cols = 512
    splits = range(len(parts))
    size_of = [p * SUB for p in parts]
    first_of = [sum(size_of[:t]) for t in splits]

    def table(values):
        found = jnp.int32(0)
        for i, v in enumerate(values):
            found = jnp.where(place == i, jnp.int32(v), found)
        return found

    at = {s: k for k, s in enumerate(order)}
    right = table([order[(at[i] + 1) % n] for i in range(n)])
    left = table([order[(at[i] - 1) % n] for i in range(n)])
    sides = (right, left)
    partner = place + 1 - 2 * odd
    ahead = lax.rem(place + 2, n)
    behind = lax.rem(place + n - 2, n)

    loads = [
        pltpu.make_async_copy(src, dst, load_sem.at[i])
        for i, (src, dst) in enumerate(
            (
                (tok_hbm, tok),
                (key_hbm, wk),
                (query_hbm, wq),
                (gate_hbm, gate),
                (up_hbm, up),
                (down_hbm, down),
                (ids_hbm, ids),
                (gain_hbm, gain),
                (decay_hbm, decay),
                (router_hbm, router),
                (carried_hbm, carried),
                (out_gain_hbm, out_gain),
            )
        )
    ]
    small = 6
    loads[small].start()
    loads[0].start()
    for copy in loads[small + 1 :]:
        copy.start()

    barrier = pltpu.get_barrier_semaphore()
    for there in (right, left, partner, ahead, behind):
        pl.semaphore_signal(barrier, inc=1, device_id={"seq": there}, device_id_type=MESH)
    for shift in range(1, groups):
        peer = lax.rem(mine + shift, groups)
        pl.semaphore_signal(barrier, inc=1, device_id={"expert": peer}, device_id_type=MESH)

    def send(src, dst, send_sem, recv_sem, **to):
        copy = pltpu.make_async_remote_copy(
            src_ref=src,
            dst_ref=dst,
            send_sem=send_sem,
            recv_sem=recv_sem,
            device_id=to,
            device_id_type=MESH,
        )
        copy.start()
        return copy

    def arrived(dst, sem):
        pltpu.make_async_copy(dst, dst, sem).wait()

    loads[small].wait()
    row_t = lax.broadcasted_iota(jnp.int32, (span, span), 0)
    col_t = lax.broadcasted_iota(jnp.int32, (span, span), 1)
    lane = lax.broadcasted_iota(jnp.int32, (span, LANES), 1)
    eye = jnp.where(row_t == col_t, 1.0, 0.0).astype(bf16)
    id_cols = dot(eye, ids[...].astype(f32).astype(bf16), (1, 1)).astype(jnp.int32)
    id0 = id_cols[:, 0:1]
    id1 = id_cols[:, 1:2]
    hits = jnp.where((lane == id0) | (lane == id1), 1.0, 0.0).astype(bf16)
    before = jnp.where(row_t > col_t, 1.0, 0.0).astype(bf16)
    slots = dot(before, hits)
    slot_s[...] = slots
    own_hit = jnp.where((ids[0:1, :] == mine) | (ids[1:2, :] == mine), 1.0, 0.0)
    own_hit = jnp.broadcast_to(own_hit, (SUB, span))
    own_slot = dot(own_hit.astype(bf16), before, (1, 1))
    want = lax.broadcasted_iota(jnp.int32, (capp, span), 0)
    picked = (own_slot[0:1, :].astype(jnp.int32) == want) & (own_hit[0:1, :] > 0.5) & (want < cap)
    select = jnp.where(picked, 1.0, 0.0).astype(bf16)

    loads[0].wait()
    loads[1].start()
    loads[2].start()
    loads[small + 1].wait()
    strip = 16

    def norm_strip(i, _):
        at_rows = pl.ds(pl.multiple_of(i * strip, strip), strip)
        x = tok[at_rows, :].astype(f32)
        scale = lax.rsqrt(jnp.mean(x * x, axis=1, keepdims=True) + norm_epsilon)
        normed[at_rows, :] = (x * scale * gain[...]).astype(bf16)
        return 0

    lax.fori_loop(0, span // strip, norm_strip, 0, unroll=4)
    loads[3].start()
    loads[4].start()
    for copy in loads[small + 2 :]:
        copy.wait()
    pl.semaphore_wait(barrier, 5 + groups - 1)
    ready_cuts = set()

    def dispatch(h):
        ready_cuts.add(h)
        for i in range(cut_cols // step_cols):
            off = i * step_cols
            got = dot(select, normed[:, h * cut_cols + off : h * cut_cols + off + step_cols])
            for t in splits:
                piece = got[first_of[t] : first_of[t] + size_of[t]].reshape(parts[t], SUB, step_cols)
                rows[t][0, h, :, :, off : off + step_cols] = piece.astype(bf16)

    plan = Plan()
    waited = set()

    def spot(rel):
        return rel % n

    def column_cut(message, side):
        kind, t, k, which = message
        return which if side == 0 else cuts - 1 - which

    def sem_of(message):
        kind, t, k, which = message
        return (ag_recv if kind == "ag" else rs_recv).at[t, (k - 1) * cuts + which]

    def need(message):
        if message in waited:
            return
        waited.add(message)
        both = inbox[message[1]].at[:, 0, 0]
        arrived(both, sem_of(message))

    def go(message):
        kind, t, k, which = message
        prev = (kind, t, k - 1 if kind == "ag" else k + 1, which)
        chained = prev in plan.arrival
        if chained:
            need(prev)
        for side in range(2):
            h = column_cut(message, side)
            if kind == "ag" and h not in ready_cuts:
                dispatch(h)
        for side in range(2):
            h = column_cut(message, side)
            if kind == "ag":
                sign = -1 if side == 0 else 1
                src = rows[t].at[spot(sign * (k - 1)), h]
                dst = rows[t].at[spot(sign * k), h]
                out = ag_send.at[t]
            else:
                rel = spot(k if side == 0 else -k)
                if chained:

                    def add_cols(i, _, side=side, h=h, rel=rel):
                        cols = pl.ds(pl.multiple_of(i * step_cols, step_cols), step_cols)
                        total = part[t][rel, h, :, :, cols].astype(f32)
                        total = total + inbox[t][side, k + 1, h, :, :, cols].astype(f32)
                        part[t][rel, h, :, :, cols] = total.astype(bf16)
                        return 0

                    lax.fori_loop(0, cut_cols // step_cols, add_cols, 0)
                src = part[t].at[rel, h]
                dst = inbox[t].at[side, k, h]
                out = rs_send.at[t]
            send(src, dst, out, sem_of(message), seq=sides[side])

    def mixing_unit():
        experts = router.shape[0]
        logits = dot(normed[...], router[...], (1, 1))
        lane_e = lax.broadcasted_iota(jnp.int32, (span, experts), 1)
        chosen0 = jnp.sum(jnp.where(lane_e == id0, logits, 0.0), axis=1, keepdims=True)
        chosen1 = jnp.sum(jnp.where(lane_e == id1, logits, 0.0), axis=1, keepdims=True)
        share0 = 1.0 / (1.0 + jnp.exp(chosen1 - chosen0))
        share1 = 1.0 - share0
        mixing = [jnp.zeros((span, groups * size), f32) for size in size_of]
        for shift in range(groups):
            source = lax.rem(mine + groups - shift, groups)
            slot = jnp.sum(jnp.where(lane == source, slot_s[...], 0.0), axis=1, keepdims=True).astype(jnp.int32)
            share = jnp.where(id0 == source, share0, jnp.where(id1 == source, share1, 0.0))
            for t in splits:
                inside = (slot >= first_of[t]) & (slot < min(first_of[t] + size_of[t], cap))
                lane_w = lax.broadcasted_iota(jnp.int32, mixing[t].shape, 1)
                here = lane_w == slot - first_of[t] + shift * size_of[t]
                mixing[t] = mixing[t] + jnp.where(here, jnp.where(inside, share, 0.0), 0.0)
        for t in splits:
            high, low = split(mixing[t])
            mix_high[t][...] = high
            mix_low[t][...] = low

    def keys_unit():
        loads[1].wait()
        ks[...] = dot(tok[...], wk[...])

    def queries_unit():
        loads[2].wait()
        qs[...] = dot(tok[...], wq[...])

    def decay_unit():
        tri = jnp.where(row_t >= col_t, 1.0, 0.0)
        run_s[...] = dot(decay[...], tri, (1, 1), exact)
        run_t[...] = dot(tri, decay[...], (1, 1), exact)
        retain_own[...] = jnp.exp(jnp.broadcast_to(run_s[:, span - 1 : span], (heads, LANES)))

    def values_of(head):
        return tok[:, pl.ds(pl.multiple_of(mine * bw + head * LANES, LANES), LANES)]

    def state_unit(p):
        tail = jnp.exp(run_t[span - 1 : span, :] - run_t[...])
        factor = jnp.zeros((span, LANES), f32)
        for a in range(per):
            inside = (lane >= a * key_size) & (lane < (a + 1) * key_size)
            factor = jnp.where(inside, tail[:, p * per + a : p * per + a + 1], factor)
        scaled = (ks[:, p * LANES : (p + 1) * LANES] * factor).T
        hi, lo = split(scaled)
        for a in range(per):
            head = p * per + a
            values = values_of(head)
            cut = slice(a * key_size, (a + 1) * key_size)
            block_state[head * key_size : (head + 1) * key_size, :] = (
                dot(hi, values) + dot(lo, values)
            )[cut]

    state_sent = []

    def pair_unit():
        pair_out[...] = block_state[...].astype(bf16)
        state_sent.append(send(pair_out, pair_in, st_send.at[0], st_recv.at[0], seq=partner))
        state_sent.append(send(retain_own, retain_in, st_send.at[1], st_recv.at[1], seq=partner))

    def chain_point(j):
        if j == 0:
            arrived(pair_in, st_recv.at[0])
            arrived(retain_in, st_recv.at[1])

        @pl.when(pair == j)
        def _():
            if j > 0:
                arrived(chain_in, st_recv.at[2])
            for head in range(heads):
                at_head = slice(head * key_size, (head + 1) * key_size)
                coming = carried[at_head, :] if j == 0 else chain_in[at_head, :].astype(f32)
                own_keep = retain_own[head : head + 1, :]
                other_keep = retain_in[head : head + 1, :]
                own = block_state[at_head, :]
                other = pair_in[at_head, :].astype(f32)
                is_odd = odd == 1
                prior[at_head, :] = jnp.where(is_odd, other_keep * coming + other, coming)
                if j < pairs - 1:
                    both = jnp.where(is_odd, own_keep * other + own, other_keep * own + other)
                    chain_out[at_head, :] = (own_keep * other_keep * coming + both).astype(bf16)
            if j < pairs - 1:
                send(chain_out, chain_in, st_send.at[2], st_recv.at[2], seq=ahead)

    def intra_unit(p):
        q_pair = qs[:, p * LANES : (p + 1) * LANES]
        k_hi, k_lo = split(ks[:, p * LANES : (p + 1) * LANES])
        for a in range(per):
            head = p * per + a
            inside = (lane >= a * key_size) & (lane < (a + 1) * key_size)
            q_hi, q_lo = split(jnp.where(inside, q_pair, 0.0))
            scores = dot(q_hi, k_hi, (1, 1)) + dot(q_hi, k_lo, (1, 1)) + dot(q_lo, k_hi, (1, 1))
            gaps = run_t[:, head : head + 1] - run_s[head : head + 1, :]
            scores = scores * jnp.where(row_t >= col_t, jnp.exp(jnp.minimum(gaps, 0.0)), 0.0)
            s_hi, s_lo = split(scores)
            values = values_of(head)
            intra[:, head * LANES : (head + 1) * LANES] = dot(s_hi, values) + dot(s_lo, values)

    def inter_unit(p):
        q_pair = qs[:, p * LANES : (p + 1) * LANES]
        s_hi, s_lo = split(prior[p * LANES : (p + 1) * LANES, :])
        for a in range(per):
            head = p * per + a
            cols = slice(head * LANES, (head + 1) * LANES)
            inside = (lane >= a * key_size) & (lane < (a + 1) * key_size)
            q_hi, q_lo = split(jnp.where(inside, q_pair, 0.0))
            carried_rows = dot(q_hi, s_hi) + dot(q_hi, s_lo) + dot(q_lo, s_hi)
            out = intra[:, cols] + jnp.exp(run_t[:, head : head + 1]) * carried_rows
            scale = lax.rsqrt(jnp.mean(out * out, axis=1, keepdims=True) + head_epsilon)
            hidden = values_of(head).astype(f32) + out * scale * out_gain[:, cols]
            intra[:, cols] = hidden
            student_out[:, cols] = hidden.astype(bf16)

    def gather_unit(b, t, members):
        def gather(i, _):
            off = pl.multiple_of(i * step_cols, step_cols)
            for h in range(cuts):
                got = [
                    rows[t][spot(rel), h, :, :, pl.ds(off, step_cols)].astype(f32).reshape(size_of[t], step_cols)
                    for rel in members
                ]
                got = jnp.concatenate(got, axis=0) if len(got) > 1 else got[0]
                lhs[0 : got.shape[0], pl.ds(h * cut_cols + off, step_cols)] = got.astype(bf16)
            return 0

        lax.fori_loop(0, cut_cols // step_cols, gather, 0)

    tile = min(256, ff)

    def hidden_unit(b, m, i):
        if b == 0 and i == 0:
            loads[3].wait()
            loads[4].wait()
        cols = slice(i * tile, (i + 1) * tile)
        a = lhs[0:m, :]
        gated = dot(a, gate[:, cols])
        upped = dot(a, up[:, cols])
        silu = gated / (1.0 + jnp.exp(-gated))
        hid[b][:, cols] = (silu * upped).astype(bf16)

    def down_unit(b, t, members, h):
        if b == 0 and h == 0:
            loads[5].wait()

        def columns(i, _):
            off = pl.multiple_of(i * step_cols, step_cols)
            got = dot(hid[b][...], down[:, pl.ds(h * cut_cols + off, step_cols)])
            for j, rel in enumerate(members):
                piece = got[j * size_of[t] : (j + 1) * size_of[t]].reshape(parts[t], SUB, step_cols)
                part[t][spot(rel), h, :, :, pl.ds(off, step_cols)] = piece.astype(bf16)
            return 0

        lax.fori_loop(0, cut_cols // step_cols, columns, 0)

    near = [0] + [s * k for k in range(1, half - 1) for s in (1, -1)]
    last = [half - 1, 1 - half, half]
    batches = [(0, near), (0, last)] + [(t, near + last) for t in splits if t > 0]

    def ag_of(t, members):
        found = []
        for rel in members:
            if rel > 0:
                found += [("ag", t, rel, w) for w in range(cuts if rel < half else cuts // 2)]
        return found

    per_cut = groups // cuts

    def finals(t):
        return [("rs", t, 1, w) for w in range(cuts)]

    def final_step(t, j):
        need(("rs", t, 1, cuts - 1 - j))
        need(("rs", t, 1, j))
        here = [q for q in range(groups) if q // per_cut in (j, cuts - 1 - j)]
        for q in here:
            h = q // per_cut
            cols = pl.ds((q % per_cut) * bw, bw)
            total = part[t][0, h, :, :, cols].astype(f32)
            total = total + inbox[t][0, 1, h, :, :, cols].astype(f32)
            total = total + inbox[t][1, 1, h, :, :, cols].astype(f32)
            expert_out[t][q] = total.astype(bf16)
        for q in here:
            shift = lax.rem(q + groups - mine, groups)

            @pl.when(mine != q)
            def _(q=q, shift=shift):
                send(expert_out[t].at[q], expert_in[t].at[shift], ex_send.at[t], ex_recv.at[t], expert=q)

    def final_sum(t):
        for j in range(cuts // 2):
            final_step(t, j)
        expert_in[t][0] = expert_out[t][mine]

    def mixed_of(t, i):
        cols = slice(i * step_cols, (i + 1) * step_cols)
        got = [
            expert_in[t][shift, :, :, cols].astype(f32).reshape(size_of[t], step_cols)
            for shift in range(groups)
        ]
        got = jnp.concatenate(got, axis=0).astype(bf16)
        return dot(mix_high[t][...], got) + dot(mix_low[t][...], got)

    def take_in(t):
        arrived(expert_in[t].at[1:groups], ex_recv.at[t])

    def mix_unit():
        for t in splits[:-1]:
            take_in(t)
        for i in range(bw // step_cols):
            cols = slice(i * step_cols, (i + 1) * step_cols)
            total = tok[:, pl.ds(pl.multiple_of(mine * bw + i * step_cols, LANES), step_cols)].astype(f32)
            for t in splits[:-1]:
                total = total + mixed_of(t, i)
            teacher[:, cols] = total

    plan.unit("keys", 0.8, keys_unit, start=3.0)
    plan.unit("decay", 0.4, decay_unit)
    state_names = []
    for p in range(heads // per):
        state_names.append(f"state{p}")
        plan.unit(f"state{p}", 0.35, functools.partial(state_unit, p), after=["keys", "decay"])
    plan.unit("pair", 0.3, pair_unit, after=state_names)
    for j in range(pairs):
        before_it = ["pair"] if j == 0 else [f"chain{j - 1}"]
        plan.unit(f"chain{j}", 0.2, functools.partial(chain_point, j), after=before_it, start=22.0 + 12.0 * j)
    plan.unit("queries", 0.8, queries_unit, start=4.0)

    def load_down():
        loads[5].start()

    plan.unit("down load", 0.0, load_down, start=8.0)
    for b, (t, members) in enumerate(batches):
        m = len(members) * size_of[t]
        share = ff / 1024
        plan.unit(
            f"gather{b}",
            0.4,
            functools.partial(
                lambda b, t, members: ([need(x) for x in ag_of(t, members)], gather_unit(b, t, members)),
                b,
                t,
                members,
            ),
            after=[f"hidden{b - 1}.{ff // tile - 1}"] if b else [],
            messages=ag_of(t, members),
        )
        for i in range(ff // tile):
            plan.unit(
                f"hidden{b}.{i}",
                max(0.85, m * 0.0054),
                functools.partial(hidden_unit, b, m, i),
                after=[f"gather{b}"] + ([f"hidden{b}.{i - 1}"] if i else []),
            )
        for h in range(cuts):
            plan.unit(
                f"down{b}.{h}",
                (2.1 + 0.005 * m) * share / cuts,
                functools.partial(down_unit, b, t, members, h),
                after=[f"hidden{b}.{ff // tile - 1}", "down load"],
            )
    plan.unit("mixing", 1.0, mixing_unit)
    for p in range(heads // per):
        plan.unit(f"intra{p}", 0.6, functools.partial(intra_unit, p), after=["keys", "queries", "decay"])
    for p in range(heads // per):
        plan.unit(
            f"inter{p}", 0.35, functools.partial(inter_unit, p), after=[f"intra{p}", f"chain{pairs - 1}"]
        )

    def ring(kind, t, k, which, needs=()):
        prev = (kind, t, k - 1 if kind == "ag" else k + 1, which)
        message = (kind, t, k, which)
        plan.message(
            message,
            size_of[t] * cut_cols * 2,
            functools.partial(go, message),
            prev if prev in plan.arrival else None,
            needs,
        )

    gathers = [
        [(t, k, w) for k in range(1, half + 1) for w in range(cuts if k < half else cuts // 2)] for t in splits
    ]
    early = gathers[0]
    rest = [x for more in gathers[1:] for x in more]
    for i, x in enumerate(early):
        ring("ag", *x)
        if i in (cuts - 1, len(early) - cuts // 2 - 1) and rest:
            for _ in range(cuts // 2):
                ring("ag", *rest.pop(0))
    for x in rest:
        ring("ag", *x)
    for t in splits:
        for k in range(half, 0, -1):
            for which in list(range(cuts // 2, cuts)) * (k < half) + list(range(cuts // 2)):
                here = [b for b, (u, members) in enumerate(batches) if u == t and k in [abs(r) for r in members]]
                both = sorted({which, cuts - 1 - which})
                ring("rs", t, k, which, [f"down{b}.{h}" for b in here for h in both])
        if t < len(parts) - 1:
            plan.unit(
                f"final{t}",
                0.2,
                functools.partial(final_sum, t),
                messages=finals(t),
                start=max(plan.arrival[m] for m in finals(t)) + 6.0,
                after=[f"down{b}.{h}" for b, (u, _) in enumerate(batches) if u == t for h in range(cuts)],
            )
    stores = [
        pltpu.make_async_copy(teacher_out, teacher_hbm, load_sem.at[0]),
        pltpu.make_async_copy(student_out, student_hbm, load_sem.at[1]),
    ]

    plan.unit(
        "store", 0.0, stores[1].start, after=[f"inter{p}" for p in range(heads // per)]
    )
    if len(parts) > 1:
        plan.unit("mix", 0.4, mix_unit, after=[f"final{len(parts) - 2}", "mixing"], start=max(plan.arrival[m] for m in finals(len(parts) - 2)) + 11.0)
    end = max(plan.arrival[m] for m in finals(len(parts) - 1))
    plan.fill(end)
    plan.drain()

    t = len(parts) - 1
    final_sum(t)
    take_in(t)
    gap_sum = jnp.zeros((span, LANES), f32)
    for i in range(bw // step_cols):
        cols = slice(i * step_cols, (i + 1) * step_cols)
        hidden = teacher[:, cols] + mixed_of(t, i)
        teacher_out[:, cols] = hidden.astype(bf16)
        gap = intra[:, cols] - hidden
        gap = gap * gap
        for c in range(step_cols // LANES):
            gap_sum = gap_sum + gap[:, c * LANES : (c + 1) * LANES]
    stores[0].start()
    loss_all[mine] = dot(jnp.ones((SUB, LANES), f32), gap_sum, (1, 1), exact)
    for shift in range(1, groups):
        peer = lax.rem(mine + shift, groups)
        send(loss_all.at[mine], loss_all.at[mine], lo_send, lo_recv, expert=peer)
    for t in splits:
        arrived(rows[t].at[0 : n - 1], ag_send.at[t])
        arrived(part[t].at[0 : n - 1], rs_send.at[t])
        arrived(expert_out[t].at[1:groups], ex_send.at[t])
    for copy in state_sent:
        copy.wait_send()

    @pl.when(pair < pairs - 1)
    def _():
        pltpu.make_async_copy(chain_out, chain_out, st_send.at[2]).wait()

    for copy in stores:
        copy.wait()
    arrived(loss_all.at[1:groups], lo_send)
    arrived(loss_all.at[1:groups], lo_recv)
    total = loss_all[0]
    for q in range(1, groups):
        total = total + loss_all[q]
    loss_out[...] = total / width


def result_kernel(teacher_in, student_in, loss_in, teacher_out, student_out, loss_out):
    teacher_out[...] = teacher_in[...]
    student_out[...] = student_in[...]
    loss_out[...] = loss_in[0:1, :]


def on_device(
    order,
    tokens,
    norm_gain,
    router_weight,
    expert_ids,
    gate_weight,
    up_weight,
    down_weight,
    query_weight,
    key_weight,
    log_decay,
    carried_state,
    out_gain,
):
    span, width = tokens.shape
    experts = router_weight.shape[1]
    groups = lax.axis_size("expert")
    cap = 7 * expert_ids.shape[1] * span // (8 * experts)
    g = -(-cap // SUB)
    n = len(order)
    half = n // 2
    ff = gate_weight.shape[2]
    bw = width // groups
    heads, key_size, feats = carried_state.shape
    keys = heads * key_size
    hbm = pl.BlockSpec(memory_space=pl.ANY)
    vmem = pl.BlockSpec(memory_space=pltpu.VMEM)
    dma = pltpu.SemaphoreType.DMA
    parts = (g - g // 2, g // 2) if g > 1 else (g,)
    sizes = [p * SUB for p in parts]
    near, last = n - 3, 3
    counts = [near * sizes[0], last * sizes[0]] + [n * size for size in sizes[1:]]

    cuts = min(4, groups) if n <= 8 else 2
    cut_cols = width // cuts

    steps = (half - 1) * cuts + cuts // 2

    scratch = [
        pltpu.VMEM((1, width), f32),
        pltpu.VMEM((experts, width), bf16),
        pltpu.VMEM(expert_ids.shape[::-1], jnp.int32),
        pltpu.VMEM(log_decay.shape, f32),
        pltpu.VMEM((keys, feats), f32),
        pltpu.VMEM((1, bw), f32),
        pltpu.VMEM((span, bw), bf16),
        pltpu.VMEM((span, bw), bf16),
        pltpu.VMEM((span, width), bf16),
        pltpu.VMEM((width, ff), bf16),
        pltpu.VMEM((width, ff), bf16),
        pltpu.VMEM((ff, width), bf16),
        pltpu.VMEM((width, keys), bf16),
        pltpu.VMEM((width, keys), bf16),
        pltpu.VMEM((span, width), bf16),
        pltpu.VMEM((max(counts), width), bf16),
        pltpu.VMEM((span, keys), f32),
        pltpu.VMEM((span, keys), f32),
        pltpu.VMEM((heads, span), f32),
        pltpu.VMEM((span, heads), f32),
        pltpu.VMEM((heads, LANES), f32),
        pltpu.VMEM((keys, feats), f32),
        pltpu.VMEM((keys, feats), f32),
        pltpu.VMEM((keys, feats), bf16),
        pltpu.VMEM((keys, feats), bf16),
        pltpu.VMEM((heads, LANES), f32),
        pltpu.VMEM((keys, feats), bf16),
        pltpu.VMEM((keys, feats), bf16),
        pltpu.VMEM((span, bw), f32),
        pltpu.VMEM((span, bw), f32),
        pltpu.VMEM((span, LANES), f32),
        pltpu.VMEM((groups, SUB, span), f32),
        [pltpu.VMEM((n, cuts, p, SUB, cut_cols), bf16) for p in parts],
        [pltpu.VMEM((n, cuts, p, SUB, cut_cols), bf16) for p in parts],
        [pltpu.VMEM((2, half + 1, cuts, p, SUB, cut_cols), bf16) for p in parts],
        [pltpu.VMEM((count, ff), bf16) for count in counts],
        [pltpu.VMEM((span, groups * size), bf16) for size in sizes],
        [pltpu.VMEM((span, groups * size), bf16) for size in sizes],
        [pltpu.VMEM((groups, p, SUB, bw), bf16) for p in parts],
        [pltpu.VMEM((groups, p, SUB, bw), bf16) for p in parts],
        dma((12,)),
        dma((len(parts),)),
        dma((len(parts), steps)),
        dma((len(parts),)),
        dma((len(parts), steps)),
        dma((3,)),
        dma((3,)),
        dma((len(parts),)),
        dma((len(parts),)),
        dma,
        dma,
    ]
    teacher, student, loss = pl.pallas_call(
        functools.partial(layer_kernel, order, cap, parts, cuts),
        out_shape=(
            jax.ShapeDtypeStruct((span, bw), bf16),
            jax.ShapeDtypeStruct((span, bw), bf16),
            jax.ShapeDtypeStruct((SUB, span), f32),
        ),
        in_specs=[hbm] * 12,
        out_specs=(hbm, hbm, vmem),
        scratch_shapes=scratch,
        compiler_params=pltpu.CompilerParams(
            collective_id=0, has_side_effects=True, vmem_limit_bytes=60 * 1024 * 1024
        ),
        name="layer",
    )(
        tokens,
        norm_gain.reshape(1, width),
        router_weight.T,
        expert_ids.T,
        gate_weight.reshape(width, ff),
        up_weight.reshape(width, ff),
        down_weight.reshape(ff, width),
        query_weight,
        key_weight,
        log_decay,
        carried_state.reshape(keys, feats),
        out_gain.reshape(1, bw),
    )
    teacher, student, loss = pl.pallas_call(
        result_kernel,
        out_shape=(
            jax.ShapeDtypeStruct((span, bw), bf16),
            jax.ShapeDtypeStruct((span, bw), bf16),
            jax.ShapeDtypeStruct((1, span), f32),
        ),
        in_specs=[vmem, vmem, vmem],
        out_specs=(vmem, vmem, vmem),
        name="result",
    )(teacher, student, loss)
    return teacher, student, loss.reshape(span)


def solution(mesh):
    return jax.shard_map(
        functools.partial(on_device, tuple(ring_order(mesh))),
        mesh=mesh,
        in_specs=(
            P("seq", None),
            P(),
            P(),
            P("seq", None),
            P("expert", None, "seq"),
            P("expert", None, "seq"),
            P("expert", "seq", None),
            P(None, "expert"),
            P(None, "expert"),
            P("expert", "seq"),
            P("expert", None, None),
            P("expert"),
        ),
        out_specs=(P("seq", "expert"), P("seq", "expert"), P("seq")),
        check_vma=False,
    )
```

```python
import functools
import jax
import jax.numpy as jnp
from jax import lax
from jax.experimental import pallas as pl
from jax.experimental.pallas import tpu as pltpu
from jax.sharding import PartitionSpec as P

norm_epsilon = 1e-05
head_epsilon = 1e-06
exact = lax.Precision.HIGHEST
f32 = jnp.float32
bf16 = jnp.bfloat16
LANES = 128
SUB = 8
MESH = pl.DeviceIdType.MESH


def ring_order(mesh):
    n = mesh.shape["seq"]
    line = mesh.devices[:, 0]
    coords = [getattr(d, "coords", None) for d in line]
    if any(c is None for c in coords):
        return list(range(n))
    places = {(c[0], c[2]): i for i, c in enumerate(coords)}
    xs = sorted({x for x, _ in places})
    zs = sorted({z for _, z in places})
    if len(places) != n or len(xs) * len(zs) != n or len(xs) % 2 or len(zs) < 2:
        return list(range(n))
    order = [places[(x, zs[0])] for x in xs]
    for turn, x in enumerate(reversed(xs)):
        column = zs[1:] if turn % 2 == 0 else zs[:0:-1]
        order += [places[(x, z)] for z in column]
    return order


def split(value):
    high = value.astype(bf16)
    low = (value - high.astype(f32)).astype(bf16)
    return high, low


def dot(a, b, dims=(1, 0), precision=None):
    return lax.dot_general(
        a,
        b,
        (((dims[0],), (dims[1],)), ((), ())),
        preferred_element_type=f32,
        precision=precision,
    )


class Plan:
    link_rate = 45000.0
    latency = 2.8

    def __init__(self):
        self.now = 0.0
        self.free = 0.0
        self.arrival = {}
        self.units = []
        self.done = set()

    def unit(self, name, cost, work, after=(), messages=(), start=0.0):
        self.units.append((name, cost, work, tuple(after), tuple(messages), start))

    def ready(self, unit):
        name, cost, work, after, messages, start = unit
        if any(a not in self.done for a in after) or any(m not in self.arrival for m in messages):
            return None
        return max([start] + [self.arrival[m] + 1.0 for m in messages])

    def run(self, unit):
        name, cost, work, after, messages, start = unit
        self.units.remove(unit)
        for a in after:
            self.force(a)
        self.now = max([self.now] + [self.arrival[m] for m in messages])
        work()
        self.now += cost
        self.done.add(name)

    def force(self, name):
        for unit in self.units:
            if unit[0] == name:
                self.run(unit)
                return
        assert name in self.done

    def fill(self, until):
        while True:
            for unit in self.units:
                when = self.ready(unit)
                if when is not None and when <= self.now and self.now + unit[1] <= until:
                    self.run(unit)
                    break
            else:
                later = [self.ready(u) for u in self.units]
                later = [w for w in later if w is not None and self.now < w < until]
                if not later:
                    return
                self.now = min(later)

    def message(self, name, size, work, before=None, needs=()):
        for a in needs:
            self.force(a)
        ready = self.arrival[before] if before is not None else self.now
        self.fill(max(ready, self.free - 0.5))
        self.now = max(self.now, ready)
        work()
        self.now += 0.1
        self.free = max(self.free, self.now) + size / self.link_rate
        self.arrival[name] = self.free + self.latency

    def drain(self):
        while self.units:
            known = [(self.ready(u), i) for i, u in enumerate(self.units)]
            known = [w for w in known if w[0] is not None]
            self.run(self.units[min(known)[1]])


def layer_kernel(
    order,
    cap,
    parts,
    cuts,
    tok_hbm,
    gain_hbm,
    router_hbm,
    ids_hbm,
    gate_hbm,
    up_hbm,
    down_hbm,
    query_hbm,
    key_hbm,
    decay_hbm,
    carried_hbm,
    out_gain_hbm,
    teacher_out,
    student_out,
    loss_out,
    gain,
    router,
    ids,
    decay,
    carried,
    out_gain,
    tok,
    gate,
    up,
    down,
    wq,
    wk,
    normed,
    lhs,
    qs,
    ks,
    run_s,
    run_t,
    retain_own,
    block_state,
    prior,
    pair_out,
    pair_in,
    retain_in,
    chain_out,
    chain_in,
    relay_out,
    relay_in,
    intra,
    teacher,
    slot_s,
    loss_all,
    rows,
    part,
    inbox,
    hid,
    mix_high,
    mix_low,
    expert_out,
    expert_in,
    load_sem,
    ag_send,
    ag_recv,
    rs_send,
    rs_recv,
    st_send,
    st_recv,
    ex_send,
    ex_recv,
    lo_send,
    lo_recv,
):
    n = len(order)
    half = n // 2
    span, width = tok.shape
    cut_cols = width // cuts
    ff = gate.shape[1]
    groups = lax.axis_size("expert")
    bw = width // groups
    capp = sum(parts) * SUB
    heads = decay.shape[0]
    key_size = block_state.shape[0] // heads
    per = LANES // key_size
    place = lax.axis_index("seq")
    mine = lax.axis_index("expert")
    pairs = n // 2
    pair = place // 2
    odd = place % 2
    step_cols = 512
    splits = range(len(parts))
    size_of = [p * SUB for p in parts]
    first_of = [sum(size_of[:t]) for t in splits]

    def table(values):
        found = jnp.int32(0)
        for i, v in enumerate(values):
            found = jnp.where(place == i, jnp.int32(v), found)
        return found

    at = {s: k for k, s in enumerate(order)}
    right = table([order[(at[i] + 1) % n] for i in range(n)])
    left = table([order[(at[i] - 1) % n] for i in range(n)])
    sides = (right, left)
    partner = place + 1 - 2 * odd
    ahead = lax.rem(place + 2, n)
    behind = lax.rem(place + n - 2, n)

    loads = [
        pltpu.make_async_copy(src, dst, load_sem.at[i])
        for i, (src, dst) in enumerate(
            (
                (tok_hbm, tok),
                (key_hbm, wk),
                (query_hbm, wq),
                (gate_hbm, gate),
                (up_hbm, up),
                (down_hbm, down),
                (ids_hbm, ids),
                (gain_hbm, gain),
                (decay_hbm, decay),
                (router_hbm, router),
                (carried_hbm, carried),
                (out_gain_hbm, out_gain),
            )
        )
    ]
    small = 6
    loads[small].start()
    loads[0].start()
    for copy in loads[small + 1 :]:
        copy.start()

    barrier = pltpu.get_barrier_semaphore()
    for there in (right, left, partner, ahead, behind):
        pl.semaphore_signal(barrier, inc=1, device_id={"seq": there}, device_id_type=MESH)
    for shift in range(1, groups):
        peer = lax.rem(mine + shift, groups)
        pl.semaphore_signal(barrier, inc=1, device_id={"expert": peer}, device_id_type=MESH)

    def send(src, dst, send_sem, recv_sem, **to):
        copy = pltpu.make_async_remote_copy(
            src_ref=src,
            dst_ref=dst,
            send_sem=send_sem,
            recv_sem=recv_sem,
            device_id=to,
            device_id_type=MESH,
        )
        copy.start()
        return copy

    def arrived(dst, sem):
        pltpu.make_async_copy(dst, dst, sem).wait()

    loads[small].wait()
    row_t = lax.broadcasted_iota(jnp.int32, (span, span), 0)
    col_t = lax.broadcasted_iota(jnp.int32, (span, span), 1)
    lane = lax.broadcasted_iota(jnp.int32, (span, LANES), 1)
    eye = jnp.where(row_t == col_t, 1.0, 0.0).astype(bf16)
    id_cols = dot(eye, ids[...].astype(f32).astype(bf16), (1, 1)).astype(jnp.int32)
    id0 = id_cols[:, 0:1]
    id1 = id_cols[:, 1:2]
    hits = jnp.where((lane == id0) | (lane == id1), 1.0, 0.0).astype(bf16)
    before = jnp.where(row_t > col_t, 1.0, 0.0).astype(bf16)
    slots = dot(before, hits)
    slot_s[...] = slots
    own_hit = jnp.where((ids[0:1, :] == mine) | (ids[1:2, :] == mine), 1.0, 0.0)
    own_hit = jnp.broadcast_to(own_hit, (SUB, span))
    own_slot = dot(own_hit.astype(bf16), before, (1, 1))
    want = lax.broadcasted_iota(jnp.int32, (capp, span), 0)
    picked = (own_slot[0:1, :].astype(jnp.int32) == want) & (own_hit[0:1, :] > 0.5) & (want < cap)
    select = jnp.where(picked, 1.0, 0.0).astype(bf16)

    loads[0].wait()
    loads[1].start()
    loads[2].start()
    loads[small + 1].wait()
    strip = 16

    def norm_strip(i, _):
        at_rows = pl.ds(pl.multiple_of(i * strip, strip), strip)
        x = tok[at_rows, :].astype(f32)
        scale = lax.rsqrt(jnp.mean(x * x, axis=1, keepdims=True) + norm_epsilon)
        normed[at_rows, :] = (x * scale * gain[...]).astype(bf16)
        return 0

    lax.fori_loop(0, span // strip, norm_strip, 0, unroll=4)
    loads[3].start()
    loads[4].start()
    for copy in loads[small + 2 :]:
        copy.wait()
    pl.semaphore_wait(barrier, 5 + groups - 1)
    ready_cuts = set()

    def dispatch(h):
        ready_cuts.add(h)
        for i in range(cut_cols // step_cols):
            off = i * step_cols
            got = dot(select, normed[:, h * cut_cols + off : h * cut_cols + off + step_cols])
            for t in splits:
                piece = got[first_of[t] : first_of[t] + size_of[t]].reshape(parts[t], SUB, step_cols)
                rows[t][0, h, :, :, off : off + step_cols] = piece.astype(bf16)

    plan = Plan()
    waited = set()

    def spot(rel):
        return rel % n

    def column_cut(message, side):
        kind, t, k, which = message
        return which if side == 0 else cuts - 1 - which

    def sem_of(message):
        kind, t, k, which = message
        return (ag_recv if kind == "ag" else rs_recv).at[t, (k - 1) * cuts + which]

    def need(message):
        if message in waited:
            return
        waited.add(message)
        both = inbox[message[1]].at[:, 0, 0]
        arrived(both, sem_of(message))

    def go(message):
        kind, t, k, which = message
        prev = (kind, t, k - 1 if kind == "ag" else k + 1, which)
        chained = prev in plan.arrival
        if chained:
            need(prev)
        for side in range(2):
            h = column_cut(message, side)
            if kind == "ag" and h not in ready_cuts:
                dispatch(h)
        for side in range(2):
            h = column_cut(message, side)
            if kind == "ag":
                sign = -1 if side == 0 else 1
                src = rows[t].at[spot(sign * (k - 1)), h]
                dst = rows[t].at[spot(sign * k), h]
                out = ag_send.at[t]
            else:
                rel = spot(k if side == 0 else -k)
                if chained:

                    def add_cols(i, _, side=side, h=h, rel=rel):
                        cols = pl.ds(pl.multiple_of(i * step_cols, step_cols), step_cols)
                        total = part[t][rel, h, :, :, cols].astype(f32)
                        total = total + inbox[t][side, k + 1, h, :, :, cols].astype(f32)
                        part[t][rel, h, :, :, cols] = total.astype(bf16)
                        return 0

                    lax.fori_loop(0, cut_cols // step_cols, add_cols, 0)
                src = part[t].at[rel, h]
                dst = inbox[t].at[side, k, h]
                out = rs_send.at[t]
            send(src, dst, out, sem_of(message), seq=sides[side])

    def mixing_unit():
        experts = router.shape[0]
        logits = dot(normed[...], router[...], (1, 1))
        lane_e = lax.broadcasted_iota(jnp.int32, (span, experts), 1)
        chosen0 = jnp.sum(jnp.where(lane_e == id0, logits, 0.0), axis=1, keepdims=True)
        chosen1 = jnp.sum(jnp.where(lane_e == id1, logits, 0.0), axis=1, keepdims=True)
        share0 = 1.0 / (1.0 + jnp.exp(chosen1 - chosen0))
        share1 = 1.0 - share0
        mixing = [jnp.zeros((span, groups * size), f32) for size in size_of]
        for shift in range(groups):
            source = lax.rem(mine + groups - shift, groups)
            slot = jnp.sum(jnp.where(lane == source, slot_s[...], 0.0), axis=1, keepdims=True).astype(jnp.int32)
            share = jnp.where(id0 == source, share0, jnp.where(id1 == source, share1, 0.0))
            for t in splits:
                inside = (slot >= first_of[t]) & (slot < min(first_of[t] + size_of[t], cap))
                lane_w = lax.broadcasted_iota(jnp.int32, mixing[t].shape, 1)
                here = lane_w == slot - first_of[t] + shift * size_of[t]
                mixing[t] = mixing[t] + jnp.where(here, jnp.where(inside, share, 0.0), 0.0)
        for t in splits:
            high, low = split(mixing[t])
            mix_high[t][...] = high
            mix_low[t][...] = low

    def keys_unit():
        loads[1].wait()
        ks[...] = dot(tok[...], wk[...])

    def queries_unit():
        loads[2].wait()
        qs[...] = dot(tok[...], wq[...])

    def decay_unit():
        tri = jnp.where(row_t >= col_t, 1.0, 0.0)
        run_s[...] = dot(decay[...], tri, (1, 1), exact)
        run_t[...] = dot(tri, decay[...], (1, 1), exact)
        retain_own[...] = jnp.exp(jnp.broadcast_to(run_s[:, span - 1 : span], (heads, LANES)))

    def values_of(head):
        return tok[:, pl.ds(pl.multiple_of(mine * bw + head * LANES, LANES), LANES)]

    def state_unit(p):
        tail = jnp.exp(run_t[span - 1 : span, :] - run_t[...])
        factor = jnp.zeros((span, LANES), f32)
        for a in range(per):
            inside = (lane >= a * key_size) & (lane < (a + 1) * key_size)
            factor = jnp.where(inside, tail[:, p * per + a : p * per + a + 1], factor)
        scaled = (ks[:, p * LANES : (p + 1) * LANES] * factor).T
        hi, lo = split(scaled)
        for a in range(per):
            head = p * per + a
            values = values_of(head)
            cut = slice(a * key_size, (a + 1) * key_size)
            block_state[head * key_size : (head + 1) * key_size, :] = (
                dot(hi, values) + dot(lo, values)
            )[cut]

    hk = heads * key_size // 2
    half_heads = heads // 2
    own_half = pl.ds(pl.multiple_of(odd * hk, key_size), hk)
    other_half = pl.ds(pl.multiple_of((1 - odd) * hk, key_size), hk)
    gives = (pair < pairs - 1) | (odd == 0)

    def pair_unit():
        pair_out[...] = block_state[other_half, :].astype(bf16)

        @pl.when(gives)
        def _():
            send(pair_out, pair_in, st_send.at[0], st_recv.at[0], seq=partner)
            send(retain_own, retain_in, st_send.at[1], st_recv.at[1], seq=partner)

    def chain_point(j):
        last_pair = j == pairs - 1

        def pair_wait():
            arrived(pair_in, st_recv.at[0])
            arrived(retain_in, st_recv.at[1])

        @pl.when(pair == j)
        def _():
            if last_pair:
                pl.when(odd == 1)(pair_wait)
            else:
                pair_wait()
            if j > 0:
                arrived(chain_in, st_recv.at[2])
            is_odd = odd == 1
            for i in range(half_heads):
                rows_i = slice(i * key_size, (i + 1) * key_size)
                at_i = pl.ds(pl.multiple_of(odd * hk + i * key_size, key_size), key_size)
                head = pl.ds(odd * half_heads + i, 1)
                coming = carried[at_i, :] if j == 0 else chain_in[rows_i, :].astype(f32)
                own_keep = retain_own[head, :]
                other_keep = retain_in[head, :]
                own = block_state[at_i, :]
                other = pair_in[rows_i, :].astype(f32)
                later = jnp.where(is_odd, other_keep * coming + other, own_keep * coming + own)
                prior[at_i, :] = jnp.where(is_odd, later, coming)
                relay_out[rows_i, :] = jnp.where(is_odd, coming, later).astype(bf16)
                if not last_pair:
                    beyond = jnp.where(is_odd, own_keep * later + own, other_keep * later + other)
                    chain_out[rows_i, :] = beyond.astype(bf16)
            send(relay_out, relay_in, st_send.at[3], st_recv.at[3], seq=partner)
            if not last_pair:
                send(chain_out, chain_in, st_send.at[2], st_recv.at[2], seq=ahead)

    def relay_unit():
        arrived(relay_in, st_recv.at[3])
        prior[other_half, :] = relay_in[...].astype(f32)

    def intra_unit(p):
        q_pair = qs[:, p * LANES : (p + 1) * LANES]
        k_hi, k_lo = split(ks[:, p * LANES : (p + 1) * LANES])
        for a in range(per):
            head = p * per + a
            inside = (lane >= a * key_size) & (lane < (a + 1) * key_size)
            q_hi, q_lo = split(jnp.where(inside, q_pair, 0.0))
            scores = dot(q_hi, k_hi, (1, 1)) + dot(q_hi, k_lo, (1, 1)) + dot(q_lo, k_hi, (1, 1))
            gaps = run_t[:, head : head + 1] - run_s[head : head + 1, :]
            scores = scores * jnp.where(row_t >= col_t, jnp.exp(jnp.minimum(gaps, 0.0)), 0.0)
            s_hi, s_lo = split(scores)
            values = values_of(head)
            intra[:, head * LANES : (head + 1) * LANES] = dot(s_hi, values) + dot(s_lo, values)

    def inter_unit(p):
        q_pair = qs[:, p * LANES : (p + 1) * LANES]
        s_hi, s_lo = split(prior[p * LANES : (p + 1) * LANES, :])
        for a in range(per):
            head = p * per + a
            cols = slice(head * LANES, (head + 1) * LANES)
            inside = (lane >= a * key_size) & (lane < (a + 1) * key_size)
            q_hi, q_lo = split(jnp.where(inside, q_pair, 0.0))
            carried_rows = dot(q_hi, s_hi) + dot(q_hi, s_lo) + dot(q_lo, s_hi)
            out = intra[:, cols] + jnp.exp(run_t[:, head : head + 1]) * carried_rows
            scale = lax.rsqrt(jnp.mean(out * out, axis=1, keepdims=True) + head_epsilon)
            hidden = values_of(head).astype(f32) + out * scale * out_gain[:, cols]
            intra[:, cols] = hidden
            student_out[:, cols] = hidden.astype(bf16)

    def gather_unit(b, t, members):
        def gather(i, _):
            off = pl.multiple_of(i * step_cols, step_cols)
            for h in range(cuts):
                got = [
                    rows[t][spot(rel), h, :, :, pl.ds(off, step_cols)].astype(f32).reshape(size_of[t], step_cols)
                    for rel in members
                ]
                got = jnp.concatenate(got, axis=0) if len(got) > 1 else got[0]
                lhs[0 : got.shape[0], pl.ds(h * cut_cols + off, step_cols)] = got.astype(bf16)
            return 0

        lax.fori_loop(0, cut_cols // step_cols, gather, 0)

    tile = min(256, ff)

    def hidden_unit(b, m, i):
        if b == 0 and i == 0:
            loads[3].wait()
            loads[4].wait()
        cols = slice(i * tile, (i + 1) * tile)
        a = lhs[0:m, :]
        gated = dot(a, gate[:, cols])
        upped = dot(a, up[:, cols])
        silu = gated / (1.0 + jnp.exp(-gated))
        hid[b][:, cols] = (silu * upped).astype(bf16)

    def down_unit(b, t, members, h):
        if b == 0 and h == 0:
            loads[5].wait()

        def columns(i, _):
            off = pl.multiple_of(i * step_cols, step_cols)
            got = dot(hid[b][...], down[:, pl.ds(h * cut_cols + off, step_cols)])
            for j, rel in enumerate(members):
                piece = got[j * size_of[t] : (j + 1) * size_of[t]].reshape(parts[t], SUB, step_cols)
                part[t][spot(rel), h, :, :, pl.ds(off, step_cols)] = piece.astype(bf16)
            return 0

        lax.fori_loop(0, cut_cols // step_cols, columns, 0)

    near = [0] + [s * k for k in range(1, half - 1) for s in (1, -1)]
    last = [half - 1, 1 - half, half]
    batches = [(0, near), (0, last)] + [(t, near + last) for t in splits if t > 0]

    def ag_of(t, members):
        found = []
        for rel in members:
            if rel > 0:
                found += [("ag", t, rel, w) for w in range(cuts if rel < half else cuts // 2)]
        return found

    per_cut = groups // cuts

    def finals(t):
        return [("rs", t, 1, w) for w in range(cuts)]

    def final_step(t, j):
        need(("rs", t, 1, cuts - 1 - j))
        need(("rs", t, 1, j))
        here = [q for q in range(groups) if q // per_cut in (j, cuts - 1 - j)]
        for q in here:
            h = q // per_cut
            cols = pl.ds((q % per_cut) * bw, bw)
            total = part[t][0, h, :, :, cols].astype(f32)
            total = total + inbox[t][0, 1, h, :, :, cols].astype(f32)
            total = total + inbox[t][1, 1, h, :, :, cols].astype(f32)
            expert_out[t][q] = total.astype(bf16)
        for q in here:
            shift = lax.rem(q + groups - mine, groups)

            @pl.when(mine != q)
            def _(q=q, shift=shift):
                send(expert_out[t].at[q], expert_in[t].at[shift], ex_send.at[t], ex_recv.at[t], expert=q)

    def final_sum(t):
        for j in range(cuts // 2):
            final_step(t, j)
        expert_in[t][0] = expert_out[t][mine]

    def mixed_of(t, i):
        cols = slice(i * step_cols, (i + 1) * step_cols)
        got = [
            expert_in[t][shift, :, :, cols].astype(f32).reshape(size_of[t], step_cols)
            for shift in range(groups)
        ]
        got = jnp.concatenate(got, axis=0).astype(bf16)
        return dot(mix_high[t][...], got) + dot(mix_low[t][...], got)

    def take_in(t):
        arrived(expert_in[t].at[1:groups], ex_recv.at[t])

    def mix_unit():
        for t in splits[:-1]:
            take_in(t)
        for i in range(bw // step_cols):
            cols = slice(i * step_cols, (i + 1) * step_cols)
            total = tok[:, pl.ds(pl.multiple_of(mine * bw + i * step_cols, LANES), step_cols)].astype(f32)
            for t in splits[:-1]:
                total = total + mixed_of(t, i)
            teacher[:, cols] = total

    plan.unit("keys", 0.8, keys_unit, start=3.0)
    plan.unit("decay", 0.4, decay_unit)
    state_names = []
    for p in range(heads // per):
        state_names.append(f"state{p}")
        plan.unit(f"state{p}", 0.35, functools.partial(state_unit, p), after=["keys", "decay"])
    plan.unit("pair", 0.3, pair_unit, after=state_names)
    for j in range(pairs):
        before_it = ["pair"] if j == 0 else [f"chain{j - 1}"]
        plan.unit(f"chain{j}", 0.2, functools.partial(chain_point, j), after=before_it, start=22.0 + 12.0 * j)
    plan.unit("relay", 0.1, relay_unit, after=[f"chain{pairs - 1}"], start=34.0 + 12.0 * (pairs - 1))
    plan.unit("queries", 0.8, queries_unit, start=4.0)

    def load_down():
        loads[5].start()

    plan.unit("down load", 0.0, load_down, start=8.0)
    for b, (t, members) in enumerate(batches):
        m = len(members) * size_of[t]
        share = ff / 1024
        plan.unit(
            f"gather{b}",
            0.4,
            functools.partial(
                lambda b, t, members: ([need(x) for x in ag_of(t, members)], gather_unit(b, t, members)),
                b,
                t,
                members,
            ),
            after=[f"hidden{b - 1}.{ff // tile - 1}"] if b else [],
            messages=ag_of(t, members),
        )
        for i in range(ff // tile):
            plan.unit(
                f"hidden{b}.{i}",
                max(0.85, m * 0.0054),
                functools.partial(hidden_unit, b, m, i),
                after=[f"gather{b}"] + ([f"hidden{b}.{i - 1}"] if i else []),
            )
        for h in range(cuts):
            plan.unit(
                f"down{b}.{h}",
                (2.1 + 0.005 * m) * share / cuts,
                functools.partial(down_unit, b, t, members, h),
                after=[f"hidden{b}.{ff // tile - 1}", "down load"],
            )
    plan.unit("mixing", 1.0, mixing_unit)
    for p in range(heads // per):
        plan.unit(f"intra{p}", 0.6, functools.partial(intra_unit, p), after=["keys", "queries", "decay"])
    for p in range(heads // per):
        plan.unit(
            f"inter{p}", 0.35, functools.partial(inter_unit, p), after=[f"intra{p}", "relay"]
        )

    def ring(kind, t, k, which, needs=()):
        prev = (kind, t, k - 1 if kind == "ag" else k + 1, which)
        message = (kind, t, k, which)
        plan.message(
            message,
            size_of[t] * cut_cols * 2,
            functools.partial(go, message),
            prev if prev in plan.arrival else None,
            needs,
        )

    gathers = [
        [(t, k, w) for k in range(1, half + 1) for w in range(cuts if k < half else cuts // 2)] for t in splits
    ]
    early = gathers[0]
    rest = [x for more in gathers[1:] for x in more]
    for i, x in enumerate(early):
        ring("ag", *x)
        if i in (cuts - 1, len(early) - cuts // 2 - 1) and rest:
            for _ in range(cuts // 2):
                ring("ag", *rest.pop(0))
    for x in rest:
        ring("ag", *x)
    for t in splits:
        for k in range(half, 0, -1):
            for which in list(range(cuts // 2, cuts)) * (k < half) + list(range(cuts // 2)):
                here = [b for b, (u, members) in enumerate(batches) if u == t and k in [abs(r) for r in members]]
                both = sorted({which, cuts - 1 - which})
                ring("rs", t, k, which, [f"down{b}.{h}" for b in here for h in both])
        if t < len(parts) - 1:
            plan.unit(
                f"final{t}",
                0.2,
                functools.partial(final_sum, t),
                messages=finals(t),
                start=max(plan.arrival[m] for m in finals(t)) + 6.0,
                after=[f"down{b}.{h}" for b, (u, _) in enumerate(batches) if u == t for h in range(cuts)],
            )
    if len(parts) > 1:
        plan.unit("mix", 0.4, mix_unit, after=[f"final{len(parts) - 2}", "mixing"], start=max(plan.arrival[m] for m in finals(len(parts) - 2)) + 11.0)
    end = max(plan.arrival[m] for m in finals(len(parts) - 1))
    plan.fill(end)
    plan.drain()

    t = len(parts) - 1
    final_sum(t)
    take_in(t)
    gap_sum = jnp.zeros((span, LANES), f32)
    for i in range(bw // step_cols):
        cols = slice(i * step_cols, (i + 1) * step_cols)
        hidden = teacher[:, cols] + mixed_of(t, i)
        teacher_out[:, cols] = hidden.astype(bf16)
        gap = intra[:, cols] - hidden
        gap = gap * gap
        for c in range(step_cols // LANES):
            gap_sum = gap_sum + gap[:, c * LANES : (c + 1) * LANES]
    loss_all[mine] = dot(jnp.ones((SUB, LANES), f32), gap_sum, (1, 1), exact)
    for shift in range(1, groups):
        peer = lax.rem(mine + shift, groups)
        send(loss_all.at[mine], loss_all.at[mine], lo_send, lo_recv, expert=peer)
    for t in splits:
        arrived(rows[t].at[0 : n - 1], ag_send.at[t])
        arrived(part[t].at[0 : n - 1], rs_send.at[t])
        arrived(expert_out[t].at[1:groups], ex_send.at[t])
    arrived(relay_out, st_send.at[3])

    @pl.when(gives)
    def _():
        arrived(pair_out, st_send.at[0])
        arrived(retain_own, st_send.at[1])

    @pl.when(pair < pairs - 1)
    def _():
        arrived(chain_out, st_send.at[2])

    arrived(loss_all.at[1:groups], lo_send)
    arrived(loss_all.at[1:groups], lo_recv)
    total = loss_all[0]
    for q in range(1, groups):
        total = total + loss_all[q]
    loss_out[...] = total[0:1, :] / width


def result_kernel(teacher_in, student_in, loss_in, teacher_out, student_out, loss_out, sems):
    copies = [
        pltpu.make_async_copy(src, dst, sems.at[i])
        for i, (src, dst) in enumerate(
            ((teacher_in, teacher_out), (student_in, student_out), (loss_in, loss_out))
        )
    ]
    for copy in copies:
        copy.start()
    for copy in copies:
        copy.wait()


def on_device(
    order,
    tokens,
    norm_gain,
    router_weight,
    expert_ids,
    gate_weight,
    up_weight,
    down_weight,
    query_weight,
    key_weight,
    log_decay,
    carried_state,
    out_gain,
):
    span, width = tokens.shape
    experts = router_weight.shape[1]
    groups = lax.axis_size("expert")
    cap = 7 * expert_ids.shape[1] * span // (8 * experts)
    g = -(-cap // SUB)
    n = len(order)
    half = n // 2
    ff = gate_weight.shape[2]
    bw = width // groups
    heads, key_size, feats = carried_state.shape
    keys = heads * key_size
    hbm = pl.BlockSpec(memory_space=pl.ANY)
    vmem = pl.BlockSpec(memory_space=pltpu.VMEM)
    dma = pltpu.SemaphoreType.DMA
    parts = (g - g // 2, g // 2) if g > 1 else (g,)
    sizes = [p * SUB for p in parts]
    near, last = n - 3, 3
    counts = [near * sizes[0], last * sizes[0]] + [n * size for size in sizes[1:]]

    cuts = min(4, groups) if n <= 8 else 2
    cut_cols = width // cuts

    steps = (half - 1) * cuts + cuts // 2

    scratch = [
        pltpu.VMEM((1, width), f32),
        pltpu.VMEM((experts, width), bf16),
        pltpu.VMEM(expert_ids.shape[::-1], jnp.int32),
        pltpu.VMEM(log_decay.shape, f32),
        pltpu.VMEM((keys, feats), f32),
        pltpu.VMEM((1, bw), f32),
        pltpu.VMEM((span, width), bf16),
        pltpu.VMEM((width, ff), bf16),
        pltpu.VMEM((width, ff), bf16),
        pltpu.VMEM((ff, width), bf16),
        pltpu.VMEM((width, keys), bf16),
        pltpu.VMEM((width, keys), bf16),
        pltpu.VMEM((span, width), bf16),
        pltpu.VMEM((max(counts), width), bf16),
        pltpu.VMEM((span, keys), f32),
        pltpu.VMEM((span, keys), f32),
        pltpu.VMEM((heads, span), f32),
        pltpu.VMEM((span, heads), f32),
        pltpu.VMEM((heads, LANES), f32),
        pltpu.VMEM((keys, feats), f32),
        pltpu.VMEM((keys, feats), f32),
        pltpu.VMEM((keys // 2, feats), bf16),
        pltpu.VMEM((keys // 2, feats), bf16),
        pltpu.VMEM((heads, LANES), f32),
        pltpu.VMEM((keys // 2, feats), bf16),
        pltpu.VMEM((keys // 2, feats), bf16),
        pltpu.VMEM((keys // 2, feats), bf16),
        pltpu.VMEM((keys // 2, feats), bf16),
        pltpu.VMEM((span, bw), f32),
        pltpu.VMEM((span, bw), f32),
        pltpu.VMEM((span, LANES), f32),
        pltpu.VMEM((groups, SUB, span), f32),
        [pltpu.VMEM((n, cuts, p, SUB, cut_cols), bf16) for p in parts],
        [pltpu.VMEM((n, cuts, p, SUB, cut_cols), bf16) for p in parts],
        [pltpu.VMEM((2, half + 1, cuts, p, SUB, cut_cols), bf16) for p in parts],
        [pltpu.VMEM((count, ff), bf16) for count in counts],
        [pltpu.VMEM((span, groups * size), bf16) for size in sizes],
        [pltpu.VMEM((span, groups * size), bf16) for size in sizes],
        [pltpu.VMEM((groups, p, SUB, bw), bf16) for p in parts],
        [pltpu.VMEM((groups, p, SUB, bw), bf16) for p in parts],
        dma((12,)),
        dma((len(parts),)),
        dma((len(parts), steps)),
        dma((len(parts),)),
        dma((len(parts), steps)),
        dma((4,)),
        dma((4,)),
        dma((len(parts),)),
        dma((len(parts),)),
        dma,
        dma,
    ]
    teacher, student, loss = pl.pallas_call(
        functools.partial(layer_kernel, order, cap, parts, cuts),
        out_shape=(
            pltpu.VMEM((span, bw), bf16),
            pltpu.VMEM((span, bw), bf16),
            pltpu.VMEM((1, span), f32),
        ),
        in_specs=[hbm] * 12,
        out_specs=(vmem, vmem, vmem),
        scratch_shapes=scratch,
        compiler_params=pltpu.CompilerParams(
            collective_id=0, has_side_effects=True, vmem_limit_bytes=60 * 1024 * 1024
        ),
        name="layer",
    )(
        tokens,
        norm_gain.reshape(1, width),
        router_weight.T,
        expert_ids.T,
        gate_weight.reshape(width, ff),
        up_weight.reshape(width, ff),
        down_weight.reshape(ff, width),
        query_weight,
        key_weight,
        log_decay,
        carried_state.reshape(keys, feats),
        out_gain.reshape(1, bw),
    )
    teacher, student, loss = pl.pallas_call(
        result_kernel,
        out_shape=(
            jax.ShapeDtypeStruct((span, bw), bf16),
            jax.ShapeDtypeStruct((span, bw), bf16),
            jax.ShapeDtypeStruct((1, span), f32),
        ),
        in_specs=[vmem, vmem, vmem],
        out_specs=(hbm, hbm, hbm),
        scratch_shapes=[dma((3,))],
        name="result",
    )(*(pltpu.with_memory_space_constraint(x, pltpu.VMEM) for x in (teacher, student, loss)))
    return teacher, student, loss.reshape(span)


def solution(mesh):
    return jax.shard_map(
        functools.partial(on_device, tuple(ring_order(mesh))),
        mesh=mesh,
        in_specs=(
            P("seq", None),
            P(),
            P(),
            P("seq", None),
            P("expert", None, "seq"),
            P("expert", None, "seq"),
            P("expert", "seq", None),
            P(None, "expert"),
            P(None, "expert"),
            P("expert", "seq"),
            P("expert", None, None),
            P("expert"),
        ),
        out_specs=(P("seq", "expert"), P("seq", "expert"), P("seq")),
        check_vma=False,
    )
```

```python
import functools
import jax
import jax.numpy as jnp
from jax import lax
from jax.experimental import pallas as pl
from jax.experimental.pallas import tpu as pltpu
from jax.sharding import PartitionSpec as P

norm_epsilon = 1e-05
head_epsilon = 1e-06
exact = lax.Precision.HIGHEST
f32 = jnp.float32
bf16 = jnp.bfloat16
LANES = 128
SUB = 8
MESH = pl.DeviceIdType.MESH


def ring_order(mesh):
    n = mesh.shape["seq"]
    line = mesh.devices[:, 0]
    coords = [getattr(d, "coords", None) for d in line]
    if any(c is None for c in coords):
        return list(range(n))
    places = {(c[0], c[2]): i for i, c in enumerate(coords)}
    xs = sorted({x for x, _ in places})
    zs = sorted({z for _, z in places})
    if len(places) != n or len(xs) * len(zs) != n or len(xs) % 2 or len(zs) < 2:
        return list(range(n))
    order = [places[(x, zs[0])] for x in xs]
    for turn, x in enumerate(reversed(xs)):
        column = zs[1:] if turn % 2 == 0 else zs[:0:-1]
        order += [places[(x, z)] for z in column]
    return order


def split(value):
    high = value.astype(bf16)
    low = (value - high.astype(f32)).astype(bf16)
    return high, low


def dot(a, b, dims=(1, 0), precision=None):
    return lax.dot_general(
        a,
        b,
        (((dims[0],), (dims[1],)), ((), ())),
        preferred_element_type=f32,
        precision=precision,
    )


class Plan:
    link_rate = 45000.0
    latency = 2.8

    def __init__(self):
        self.now = 0.0
        self.free = 0.0
        self.arrival = {}
        self.units = []
        self.done = set()

    def unit(self, name, cost, work, after=(), messages=(), start=0.0):
        self.units.append((name, cost, work, tuple(after), tuple(messages), start))

    def ready(self, unit):
        name, cost, work, after, messages, start = unit
        if any(a not in self.done for a in after) or any(m not in self.arrival for m in messages):
            return None
        return max([start] + [self.arrival[m] + 1.0 for m in messages])

    def run(self, unit):
        name, cost, work, after, messages, start = unit
        self.units.remove(unit)
        for a in after:
            self.force(a)
        self.now = max([self.now] + [self.arrival[m] for m in messages])
        work()
        self.now += cost
        self.done.add(name)

    def force(self, name):
        for unit in self.units:
            if unit[0] == name:
                self.run(unit)
                return
        assert name in self.done

    def fill(self, until):
        while True:
            for unit in self.units:
                when = self.ready(unit)
                if when is not None and when <= self.now and self.now + unit[1] <= until:
                    self.run(unit)
                    break
            else:
                later = [self.ready(u) for u in self.units]
                later = [w for w in later if w is not None and self.now < w < until]
                if not later:
                    return
                self.now = min(later)

    def message(self, name, size, work, before=None, needs=()):
        for a in needs:
            self.force(a)
        ready = self.arrival[before] if before is not None else self.now
        self.fill(max(ready, self.free - 0.5))
        self.now = max(self.now, ready)
        work()
        self.now += 0.1
        self.free = max(self.free, self.now) + size / self.link_rate
        self.arrival[name] = self.free + self.latency

    def drain(self):
        while self.units:
            known = [(self.ready(u), i) for i, u in enumerate(self.units)]
            known = [w for w in known if w[0] is not None]
            self.run(self.units[min(known)[1]])


def layer_kernel(
    order,
    cap,
    parts,
    cuts,
    tok_hbm,
    gain_hbm,
    router_hbm,
    ids_hbm,
    gate_hbm,
    up_hbm,
    down_hbm,
    query_hbm,
    key_hbm,
    decay_hbm,
    carried_hbm,
    out_gain_hbm,
    teacher_out,
    student_out,
    loss_out,
    gain,
    router,
    ids,
    decay,
    carried,
    out_gain,
    tok,
    gate,
    up,
    down,
    wq,
    wk,
    normed,
    lhs,
    qs,
    ks,
    run_s,
    run_t,
    retain_own,
    block_state,
    prior,
    pair_out,
    pair_in,
    retain_in,
    chain_out,
    chain_in,
    relay_out,
    relay_in,
    intra,
    teacher,
    slot_s,
    loss_all,
    rows,
    part,
    inbox,
    hid,
    mix_high,
    mix_low,
    expert_out,
    expert_in,
    load_sem,
    ag_send,
    ag_recv,
    rs_send,
    rs_recv,
    st_send,
    st_recv,
    ex_send,
    ex_recv,
    lo_send,
    lo_recv,
    ow_recv,
):
    n = len(order)
    half = n // 2
    span, width = tok.shape
    cut_cols = width // cuts
    ff = gate.shape[1]
    groups = lax.axis_size("expert")
    bw = width // groups
    capp = sum(parts) * SUB
    heads = decay.shape[0]
    key_size = block_state.shape[0] // heads
    per = LANES // key_size
    place = lax.axis_index("seq")
    mine = lax.axis_index("expert")
    pairs = n // 2
    pair = place // 2
    odd = place % 2
    step_cols = 512
    splits = range(len(parts))
    size_of = [p * SUB for p in parts]
    first_of = [sum(size_of[:t]) for t in splits]

    def table(values):
        found = jnp.int32(0)
        for i, v in enumerate(values):
            found = jnp.where(place == i, jnp.int32(v), found)
        return found

    at = {s: k for k, s in enumerate(order)}
    right = table([order[(at[i] + 1) % n] for i in range(n)])
    left = table([order[(at[i] - 1) % n] for i in range(n)])
    sides = (right, left)
    partner = place + 1 - 2 * odd
    ahead = lax.rem(place + 2, n)
    behind = lax.rem(place + n - 2, n)

    loads = [
        pltpu.make_async_copy(src, dst, load_sem.at[i])
        for i, (src, dst) in enumerate(
            (
                (tok_hbm, tok),
                (key_hbm, wk),
                (query_hbm, wq),
                (gate_hbm, gate),
                (up_hbm, up),
                (down_hbm, down),
                (ids_hbm, ids),
                (gain_hbm, gain),
                (decay_hbm, decay),
                (router_hbm, router),
                (carried_hbm, carried),
                (out_gain_hbm, out_gain),
            )
        )
    ]
    small = 6
    loads[small].start()
    loads[0].start()
    for copy in loads[small + 1 :]:
        copy.start()

    barrier = pltpu.get_barrier_semaphore()
    for there in (partner, ahead, behind):
        pl.semaphore_signal(barrier, inc=1, device_id={"seq": there}, device_id_type=MESH)
    for there in (right, left):
        for q in range(groups):
            pl.semaphore_signal(barrier, inc=1, device_id={"seq": there, "expert": q}, device_id_type=MESH)
    for shift in range(1, groups):
        peer = lax.rem(mine + shift, groups)
        pl.semaphore_signal(barrier, inc=1, device_id={"expert": peer}, device_id_type=MESH)

    def send(src, dst, send_sem, recv_sem, **to):
        copy = pltpu.make_async_remote_copy(
            src_ref=src,
            dst_ref=dst,
            send_sem=send_sem,
            recv_sem=recv_sem,
            device_id=to,
            device_id_type=MESH,
        )
        copy.start()
        return copy

    def arrived(dst, sem):
        pltpu.make_async_copy(dst, dst, sem).wait()

    loads[small].wait()
    row_t = lax.broadcasted_iota(jnp.int32, (span, span), 0)
    col_t = lax.broadcasted_iota(jnp.int32, (span, span), 1)
    lane = lax.broadcasted_iota(jnp.int32, (span, LANES), 1)
    eye = jnp.where(row_t == col_t, 1.0, 0.0).astype(bf16)
    id_cols = dot(eye, ids[...].astype(f32).astype(bf16), (1, 1)).astype(jnp.int32)
    id0 = id_cols[:, 0:1]
    id1 = id_cols[:, 1:2]
    hits = jnp.where((lane == id0) | (lane == id1), 1.0, 0.0).astype(bf16)
    before = jnp.where(row_t > col_t, 1.0, 0.0).astype(bf16)
    slots = dot(before, hits)
    slot_s[...] = slots
    own_hit = jnp.where((ids[0:1, :] == mine) | (ids[1:2, :] == mine), 1.0, 0.0)
    own_hit = jnp.broadcast_to(own_hit, (SUB, span))
    own_slot = dot(own_hit.astype(bf16), before, (1, 1))
    want = lax.broadcasted_iota(jnp.int32, (capp, span), 0)
    picked = (own_slot[0:1, :].astype(jnp.int32) == want) & (own_hit[0:1, :] > 0.5) & (want < cap)
    select = jnp.where(picked, 1.0, 0.0).astype(bf16)

    loads[0].wait()
    loads[1].start()
    loads[2].start()
    loads[small + 1].wait()
    strip = 16

    def norm_strip(i, _):
        at_rows = pl.ds(pl.multiple_of(i * strip, strip), strip)
        x = tok[at_rows, :].astype(f32)
        scale = lax.rsqrt(jnp.mean(x * x, axis=1, keepdims=True) + norm_epsilon)
        normed[at_rows, :] = (x * scale * gain[...]).astype(bf16)
        return 0

    lax.fori_loop(0, span // strip, norm_strip, 0, unroll=4)
    loads[3].start()
    loads[4].start()
    for copy in loads[small + 2 :]:
        copy.wait()
    pl.semaphore_wait(barrier, 3 + 2 * groups + groups - 1)
    ready_cuts = set()

    def dispatch(h):
        ready_cuts.add(h)
        for i in range(cut_cols // step_cols):
            off = i * step_cols
            got = dot(select, normed[:, h * cut_cols + off : h * cut_cols + off + step_cols])
            for t in splits:
                piece = got[first_of[t] : first_of[t] + size_of[t]].reshape(parts[t], SUB, step_cols)
                rows[t][0, h, :, :, off : off + step_cols] = piece.astype(bf16)

    plan = Plan()
    waited = set()
    per_cut = groups // cuts

    def spot(rel):
        return rel % n

    def column_cut(message, side):
        kind, t, k, which = message
        return which if side == 0 else cuts - 1 - which

    def sem_of(message):
        kind, t, k, which = message
        return (ag_recv if kind == "ag" else rs_recv).at[t, (k - 1) * cuts + which]

    def need(message):
        if message in waited:
            return
        waited.add(message)
        both = inbox[message[1]].at[:, 0, 0]
        arrived(both, sem_of(message))

    def go(message):
        kind, t, k, which = message
        prev = (kind, t, k - 1 if kind == "ag" else k + 1, which)
        chained = prev in plan.arrival
        if chained:
            need(prev)
        for side in range(2):
            h = column_cut(message, side)
            if kind == "ag" and h not in ready_cuts:
                dispatch(h)
        for side in range(2):
            h = column_cut(message, side)
            if kind == "ag":
                sign = -1 if side == 0 else 1
                src = rows[t].at[spot(sign * (k - 1)), h]
                dst = rows[t].at[spot(sign * k), h]
                out = ag_send.at[t]
            else:
                rel = spot(k if side == 0 else -k)
                if chained:

                    def add_cols(i, _, side=side, h=h, rel=rel):
                        cols = pl.ds(pl.multiple_of(i * step_cols, step_cols), step_cols)
                        total = part[t][rel, h, :, :, cols].astype(f32)
                        total = total + inbox[t][side, k + 1, h, :, :, cols].astype(f32)
                        part[t][rel, h, :, :, cols] = total.astype(bf16)
                        return 0

                    lax.fori_loop(0, cut_cols // step_cols, add_cols, 0)
                if k == 1 and t == len(parts) - 1:
                    for q in range(h * per_cut, (h + 1) * per_cut):
                        piece = part[t].at[rel, h, :, :, pl.ds((q - h * per_cut) * bw, bw)]
                        there = expert_in[t].at[lax.rem(q + groups - mine, groups), side]
                        send(piece, there, rs_send.at[t], ex_recv.at[t], seq=sides[side], expert=q)
                    continue
                src = part[t].at[rel, h]
                dst = inbox[t].at[side, k, h]
                out = rs_send.at[t]
            send(src, dst, out, sem_of(message), seq=sides[side])

    def mixing_unit():
        experts = router.shape[0]
        logits = dot(normed[...], router[...], (1, 1))
        lane_e = lax.broadcasted_iota(jnp.int32, (span, experts), 1)
        chosen0 = jnp.sum(jnp.where(lane_e == id0, logits, 0.0), axis=1, keepdims=True)
        chosen1 = jnp.sum(jnp.where(lane_e == id1, logits, 0.0), axis=1, keepdims=True)
        share0 = 1.0 / (1.0 + jnp.exp(chosen1 - chosen0))
        share1 = 1.0 - share0
        mixing = [jnp.zeros((span, groups * size), f32) for size in size_of]
        for shift in range(groups):
            source = lax.rem(mine + groups - shift, groups)
            slot = jnp.sum(jnp.where(lane == source, slot_s[...], 0.0), axis=1, keepdims=True).astype(jnp.int32)
            share = jnp.where(id0 == source, share0, jnp.where(id1 == source, share1, 0.0))
            for t in splits:
                inside = (slot >= first_of[t]) & (slot < min(first_of[t] + size_of[t], cap))
                lane_w = lax.broadcasted_iota(jnp.int32, mixing[t].shape, 1)
                here = lane_w == slot - first_of[t] + shift * size_of[t]
                mixing[t] = mixing[t] + jnp.where(here, jnp.where(inside, share, 0.0), 0.0)
        for t in splits:
            high, low = split(mixing[t])
            mix_high[t][...] = high
            mix_low[t][...] = low

    def keys_unit():
        loads[1].wait()
        ks[...] = dot(tok[...], wk[...])

    def queries_unit():
        loads[2].wait()
        qs[...] = dot(tok[...], wq[...])

    def decay_unit():
        tri = jnp.where(row_t >= col_t, 1.0, 0.0)
        run_s[...] = dot(decay[...], tri, (1, 1), exact)
        run_t[...] = dot(tri, decay[...], (1, 1), exact)
        retain_own[...] = jnp.exp(jnp.broadcast_to(run_s[:, span - 1 : span], (heads, LANES)))

    def values_of(head):
        return tok[:, pl.ds(pl.multiple_of(mine * bw + head * LANES, LANES), LANES)]

    def state_unit(p):
        tail = jnp.exp(run_t[span - 1 : span, :] - run_t[...])
        factor = jnp.zeros((span, LANES), f32)
        for a in range(per):
            inside = (lane >= a * key_size) & (lane < (a + 1) * key_size)
            factor = jnp.where(inside, tail[:, p * per + a : p * per + a + 1], factor)
        scaled = (ks[:, p * LANES : (p + 1) * LANES] * factor).T
        hi, lo = split(scaled)
        for a in range(per):
            head = p * per + a
            values = values_of(head)
            cut = slice(a * key_size, (a + 1) * key_size)
            block_state[head * key_size : (head + 1) * key_size, :] = (
                dot(hi, values) + dot(lo, values)
            )[cut]

    hk = heads * key_size // 2
    half_heads = heads // 2
    own_half = pl.ds(pl.multiple_of(odd * hk, key_size), hk)
    other_half = pl.ds(pl.multiple_of((1 - odd) * hk, key_size), hk)
    gives = (pair < pairs - 1) | (odd == 0)

    def pair_unit():
        pair_out[...] = block_state[other_half, :].astype(bf16)

        @pl.when(gives)
        def _():
            send(pair_out, pair_in, st_send.at[0], st_recv.at[0], seq=partner)
            send(retain_own, retain_in, st_send.at[1], st_recv.at[1], seq=partner)

    def chain_point(j):
        last_pair = j == pairs - 1

        def pair_wait():
            arrived(pair_in, st_recv.at[0])
            arrived(retain_in, st_recv.at[1])

        @pl.when(pair == j)
        def _():
            if last_pair:
                pl.when(odd == 1)(pair_wait)
            else:
                pair_wait()
            if j > 0:
                arrived(chain_in, st_recv.at[2])
            is_odd = odd == 1
            for i in range(half_heads):
                rows_i = slice(i * key_size, (i + 1) * key_size)
                at_i = pl.ds(pl.multiple_of(odd * hk + i * key_size, key_size), key_size)
                head = pl.ds(odd * half_heads + i, 1)
                coming = carried[at_i, :] if j == 0 else chain_in[rows_i, :].astype(f32)
                own_keep = retain_own[head, :]
                other_keep = retain_in[head, :]
                own = block_state[at_i, :]
                other = pair_in[rows_i, :].astype(f32)
                later = jnp.where(is_odd, other_keep * coming + other, own_keep * coming + own)
                prior[at_i, :] = jnp.where(is_odd, later, coming)
                relay_out[rows_i, :] = jnp.where(is_odd, coming, later).astype(bf16)
                if not last_pair:
                    beyond = jnp.where(is_odd, own_keep * later + own, other_keep * later + other)
                    chain_out[rows_i, :] = beyond.astype(bf16)
            send(relay_out, relay_in, st_send.at[3], st_recv.at[3], seq=partner)
            if not last_pair:
                send(chain_out, chain_in, st_send.at[2], st_recv.at[2], seq=ahead)

    def relay_unit():
        arrived(relay_in, st_recv.at[3])
        prior[other_half, :] = relay_in[...].astype(f32)

    def intra_unit(p):
        q_pair = qs[:, p * LANES : (p + 1) * LANES]
        k_hi, k_lo = split(ks[:, p * LANES : (p + 1) * LANES])
        for a in range(per):
            head = p * per + a
            inside = (lane >= a * key_size) & (lane < (a + 1) * key_size)
            q_hi, q_lo = split(jnp.where(inside, q_pair, 0.0))
            scores = dot(q_hi, k_hi, (1, 1)) + dot(q_hi, k_lo, (1, 1)) + dot(q_lo, k_hi, (1, 1))
            gaps = run_t[:, head : head + 1] - run_s[head : head + 1, :]
            scores = scores * jnp.where(row_t >= col_t, jnp.exp(jnp.minimum(gaps, 0.0)), 0.0)
            s_hi, s_lo = split(scores)
            values = values_of(head)
            intra[:, head * LANES : (head + 1) * LANES] = dot(s_hi, values) + dot(s_lo, values)

    def inter_unit(p):
        q_pair = qs[:, p * LANES : (p + 1) * LANES]
        s_hi, s_lo = split(prior[p * LANES : (p + 1) * LANES, :])
        for a in range(per):
            head = p * per + a
            cols = slice(head * LANES, (head + 1) * LANES)
            inside = (lane >= a * key_size) & (lane < (a + 1) * key_size)
            q_hi, q_lo = split(jnp.where(inside, q_pair, 0.0))
            carried_rows = dot(q_hi, s_hi) + dot(q_hi, s_lo) + dot(q_lo, s_hi)
            out = intra[:, cols] + jnp.exp(run_t[:, head : head + 1]) * carried_rows
            scale = lax.rsqrt(jnp.mean(out * out, axis=1, keepdims=True) + head_epsilon)
            hidden = values_of(head).astype(f32) + out * scale * out_gain[:, cols]
            intra[:, cols] = hidden
            student_out[:, cols] = hidden.astype(bf16)

    def gather_unit(b, t, members):
        def gather(i, _):
            off = pl.multiple_of(i * step_cols, step_cols)
            for h in range(cuts):
                got = [
                    rows[t][spot(rel), h, :, :, pl.ds(off, step_cols)].astype(f32).reshape(size_of[t], step_cols)
                    for rel in members
                ]
                got = jnp.concatenate(got, axis=0) if len(got) > 1 else got[0]
                lhs[0 : got.shape[0], pl.ds(h * cut_cols + off, step_cols)] = got.astype(bf16)
            return 0

        lax.fori_loop(0, cut_cols // step_cols, gather, 0)

    tile = min(256, ff)

    def hidden_unit(b, m, i):
        if b == 0 and i == 0:
            loads[3].wait()
            loads[4].wait()
        cols = slice(i * tile, (i + 1) * tile)
        a = lhs[0:m, :]
        gated = dot(a, gate[:, cols])
        upped = dot(a, up[:, cols])
        silu = gated / (1.0 + jnp.exp(-gated))
        hid[b][:, cols] = (silu * upped).astype(bf16)

    def down_unit(b, t, members, h):
        if b == 0 and h == 0:
            loads[5].wait()

        def columns(i, _):
            off = pl.multiple_of(i * step_cols, step_cols)
            got = dot(hid[b][...], down[:, pl.ds(h * cut_cols + off, step_cols)])
            for j, rel in enumerate(members):
                piece = got[j * size_of[t] : (j + 1) * size_of[t]].reshape(parts[t], SUB, step_cols)
                part[t][spot(rel), h, :, :, pl.ds(off, step_cols)] = piece.astype(bf16)
            return 0

        lax.fori_loop(0, cut_cols // step_cols, columns, 0)

    near = [0] + [s * k for k in range(1, half - 1) for s in (1, -1)]
    last = [half - 1, 1 - half, half]
    batches = [(0, near), (0, last)] + [(t, near + last) for t in splits if t > 0]

    def ag_of(t, members):
        found = []
        for rel in members:
            if rel > 0:
                found += [("ag", t, rel, w) for w in range(cuts if rel < half else cuts // 2)]
        return found

    def own_unit(t):
        for q in range(groups):
            h = q // per_cut
            shift = lax.rem(q + groups - mine, groups)
            cols = pl.ds((q - h * per_cut) * bw, bw)

            @pl.when(mine != q)
            def _(q=q, h=h, shift=shift, cols=cols):
                send(part[t].at[0, h, :, :, cols], expert_in[t].at[shift, 2], ex_send.at[t], ow_recv, expert=q)

            @pl.when(mine == q)
            def _(q=q, h=h, cols=cols):
                expert_in[t][0, 2] = part[t][0, h, :, :, cols]

    def finals(t):
        return [("rs", t, 1, w) for w in range(cuts)]

    def final_step(t, j):
        need(("rs", t, 1, cuts - 1 - j))
        need(("rs", t, 1, j))
        here = [q for q in range(groups) if q // per_cut in (j, cuts - 1 - j)]
        for q in here:
            h = q // per_cut
            cols = pl.ds((q % per_cut) * bw, bw)
            total = part[t][0, h, :, :, cols].astype(f32)
            total = total + inbox[t][0, 1, h, :, :, cols].astype(f32)
            total = total + inbox[t][1, 1, h, :, :, cols].astype(f32)
            expert_out[t][q] = total.astype(bf16)
        for q in here:
            shift = lax.rem(q + groups - mine, groups)

            @pl.when(mine != q)
            def _(q=q, shift=shift):
                send(expert_out[t].at[q], expert_in[t].at[shift], ex_send.at[t], ex_recv.at[t], expert=q)

    def final_sum(t):
        for j in range(cuts // 2):
            final_step(t, j)
        expert_in[t][0] = expert_out[t][mine]

    def mixed_of(t, i):
        cols = slice(i * step_cols, (i + 1) * step_cols)
        got = []
        for shift in range(groups):
            if t < len(parts) - 1:
                one = expert_in[t][shift, :, :, cols].astype(f32)
            else:
                one = expert_in[t][shift, 2, :, :, cols].astype(f32)
                one = one + expert_in[t][shift, 0, :, :, cols].astype(f32)
                one = one + expert_in[t][shift, 1, :, :, cols].astype(f32)
                one = one.astype(bf16).astype(f32)
            got.append(one.reshape(size_of[t], step_cols))
        got = jnp.concatenate(got, axis=0).astype(bf16)
        return dot(mix_high[t][...], got) + dot(mix_low[t][...], got)

    def take_last():
        t = len(parts) - 1
        arrived(expert_in[t].at[1:groups, 2], ow_recv)
        arrived(expert_in[t].at[:, 0:2], ex_recv.at[t])

    def take_in(t):
        arrived(expert_in[t].at[1:groups], ex_recv.at[t])

    def mix_unit():
        for t in splits[:-1]:
            take_in(t)
        for i in range(bw // step_cols):
            cols = slice(i * step_cols, (i + 1) * step_cols)
            total = tok[:, pl.ds(pl.multiple_of(mine * bw + i * step_cols, LANES), step_cols)].astype(f32)
            for t in splits[:-1]:
                total = total + mixed_of(t, i)
            teacher[:, cols] = total

    plan.unit("keys", 0.8, keys_unit, start=3.0)
    plan.unit("decay", 0.4, decay_unit)
    state_names = []
    for p in range(heads // per):
        state_names.append(f"state{p}")
        plan.unit(f"state{p}", 0.35, functools.partial(state_unit, p), after=["keys", "decay"])
    plan.unit("pair", 0.3, pair_unit, after=state_names)
    for j in range(pairs):
        before_it = ["pair"] if j == 0 else [f"chain{j - 1}"]
        plan.unit(f"chain{j}", 0.2, functools.partial(chain_point, j), after=before_it, start=22.0 + 12.0 * j)
    plan.unit("relay", 0.1, relay_unit, after=[f"chain{pairs - 1}"], start=34.0 + 12.0 * (pairs - 1))
    plan.unit("queries", 0.8, queries_unit, start=4.0)

    def load_down():
        loads[5].start()

    plan.unit("down load", 0.0, load_down, start=8.0)
    for b, (t, members) in enumerate(batches):
        m = len(members) * size_of[t]
        share = ff / 1024
        plan.unit(
            f"gather{b}",
            0.4,
            functools.partial(
                lambda b, t, members: ([need(x) for x in ag_of(t, members)], gather_unit(b, t, members)),
                b,
                t,
                members,
            ),
            after=[f"hidden{b - 1}.{ff // tile - 1}"] if b else [],
            messages=ag_of(t, members),
        )
        for i in range(ff // tile):
            plan.unit(
                f"hidden{b}.{i}",
                max(0.85, m * 0.0054),
                functools.partial(hidden_unit, b, m, i),
                after=[f"gather{b}"] + ([f"hidden{b}.{i - 1}"] if i else []),
            )
        for h in range(cuts):
            plan.unit(
                f"down{b}.{h}",
                (2.1 + 0.005 * m) * share / cuts,
                functools.partial(down_unit, b, t, members, h),
                after=[f"hidden{b}.{ff // tile - 1}", "down load"],
            )
    plan.unit("mixing", 1.0, mixing_unit)
    for p in range(heads // per):
        plan.unit(f"intra{p}", 0.6, functools.partial(intra_unit, p), after=["keys", "queries", "decay"])
    for p in range(heads // per):
        plan.unit(
            f"inter{p}", 0.35, functools.partial(inter_unit, p), after=[f"intra{p}", "relay"]
        )

    def ring(kind, t, k, which, needs=()):
        prev = (kind, t, k - 1 if kind == "ag" else k + 1, which)
        message = (kind, t, k, which)
        plan.message(
            message,
            size_of[t] * cut_cols * 2,
            functools.partial(go, message),
            prev if prev in plan.arrival else None,
            needs,
        )

    gathers = [
        [(t, k, w) for k in range(1, half + 1) for w in range(cuts if k < half else cuts // 2)] for t in splits
    ]
    early = gathers[0]
    rest = [x for more in gathers[1:] for x in more]
    for i, x in enumerate(early):
        ring("ag", *x)
        if i in (cuts - 1, len(early) - cuts // 2 - 1) and rest:
            for _ in range(cuts // 2):
                ring("ag", *rest.pop(0))
    for x in rest:
        ring("ag", *x)
    for t in splits:
        for k in range(half, 0, -1):
            for which in list(range(cuts // 2, cuts)) * (k < half) + list(range(cuts // 2)):
                here = [b for b, (u, members) in enumerate(batches) if u == t and k in [abs(r) for r in members]]
                both = sorted({which, cuts - 1 - which})
                ring("rs", t, k, which, [f"down{b}.{h}" for b in here for h in both])
        if t < len(parts) - 1:
            plan.unit(
                f"final{t}",
                0.2,
                functools.partial(final_sum, t),
                messages=finals(t),
                start=max(plan.arrival[m] for m in finals(t)) + 6.0,
                after=[f"down{b}.{h}" for b, (u, _) in enumerate(batches) if u == t for h in range(cuts)],
            )
    t = len(parts) - 1
    plan.unit(
        "own",
        0.2,
        functools.partial(own_unit, t),
        after=[f"down{b}.{h}" for b, (u, _) in enumerate(batches) if u == t for h in range(cuts)],
        start=max(plan.arrival[m] for m in finals(t)) - 12.0,
    )
    if len(parts) > 1:
        plan.unit("mix", 0.4, mix_unit, after=[f"final{len(parts) - 2}", "mixing"], start=max(plan.arrival[m] for m in finals(len(parts) - 2)) + 11.0)
    end = max(plan.arrival[m] for m in finals(len(parts) - 1))
    plan.fill(end)
    plan.drain()

    t = len(parts) - 1
    take_last()
    gap_sum = jnp.zeros((span, LANES), f32)
    for i in range(bw // step_cols):
        cols = slice(i * step_cols, (i + 1) * step_cols)
        hidden = teacher[:, cols] + mixed_of(t, i)
        teacher_out[:, cols] = hidden.astype(bf16)
        gap = intra[:, cols] - hidden
        gap = gap * gap
        for c in range(step_cols // LANES):
            gap_sum = gap_sum + gap[:, c * LANES : (c + 1) * LANES]
    loss_all[mine] = dot(jnp.ones((SUB, LANES), f32), gap_sum, (1, 1), exact)
    for shift in range(1, groups):
        peer = lax.rem(mine + shift, groups)
        send(loss_all.at[mine], loss_all.at[mine], lo_send, lo_recv, expert=peer)
    for t in splits:
        arrived(rows[t].at[0 : n - 1], ag_send.at[t])
        arrived(part[t].at[0 : n - 1], rs_send.at[t])
        arrived(expert_out[t].at[1:groups] if t < len(parts) - 1 else expert_in[t].at[1:groups, 2], ex_send.at[t])
    arrived(relay_out, st_send.at[3])

    @pl.when(gives)
    def _():
        arrived(pair_out, st_send.at[0])
        arrived(retain_own, st_send.at[1])

    @pl.when(pair < pairs - 1)
    def _():
        arrived(chain_out, st_send.at[2])

    arrived(loss_all.at[1:groups], lo_send)
    arrived(loss_all.at[1:groups], lo_recv)
    total = loss_all[0]
    for q in range(1, groups):
        total = total + loss_all[q]
    loss_out[...] = total[0:1, :] / width


def result_kernel(teacher_in, student_in, loss_in, teacher_out, student_out, loss_out, sems):
    copies = [
        pltpu.make_async_copy(src, dst, sems.at[i])
        for i, (src, dst) in enumerate(
            ((teacher_in, teacher_out), (student_in, student_out), (loss_in, loss_out))
        )
    ]
    for copy in copies:
        copy.start()
    for copy in copies:
        copy.wait()


def on_device(
    order,
    tokens,
    norm_gain,
    router_weight,
    expert_ids,
    gate_weight,
    up_weight,
    down_weight,
    query_weight,
    key_weight,
    log_decay,
    carried_state,
    out_gain,
):
    span, width = tokens.shape
    experts = router_weight.shape[1]
    groups = lax.axis_size("expert")
    cap = 7 * expert_ids.shape[1] * span // (8 * experts)
    g = -(-cap // SUB)
    n = len(order)
    half = n // 2
    ff = gate_weight.shape[2]
    bw = width // groups
    heads, key_size, feats = carried_state.shape
    keys = heads * key_size
    hbm = pl.BlockSpec(memory_space=pl.ANY)
    vmem = pl.BlockSpec(memory_space=pltpu.VMEM)
    dma = pltpu.SemaphoreType.DMA
    parts = (g - g // 2, g // 2) if g > 1 else (g,)
    sizes = [p * SUB for p in parts]
    near, last = n - 3, 3
    counts = [near * sizes[0], last * sizes[0]] + [n * size for size in sizes[1:]]

    cuts = min(4, groups) if n <= 8 else 2
    cut_cols = width // cuts

    steps = (half - 1) * cuts + cuts // 2

    scratch = [
        pltpu.VMEM((1, width), f32),
        pltpu.VMEM((experts, width), bf16),
        pltpu.VMEM(expert_ids.shape[::-1], jnp.int32),
        pltpu.VMEM(log_decay.shape, f32),
        pltpu.VMEM((keys, feats), f32),
        pltpu.VMEM((1, bw), f32),
        pltpu.VMEM((span, width), bf16),
        pltpu.VMEM((width, ff), bf16),
        pltpu.VMEM((width, ff), bf16),
        pltpu.VMEM((ff, width), bf16),
        pltpu.VMEM((width, keys), bf16),
        pltpu.VMEM((width, keys), bf16),
        pltpu.VMEM((span, width), bf16),
        pltpu.VMEM((max(counts), width), bf16),
        pltpu.VMEM((span, keys), f32),
        pltpu.VMEM((span, keys), f32),
        pltpu.VMEM((heads, span), f32),
        pltpu.VMEM((span, heads), f32),
        pltpu.VMEM((heads, LANES), f32),
        pltpu.VMEM((keys, feats), f32),
        pltpu.VMEM((keys, feats), f32),
        pltpu.VMEM((keys // 2, feats), bf16),
        pltpu.VMEM((keys // 2, feats), bf16),
        pltpu.VMEM((heads, LANES), f32),
        pltpu.VMEM((keys // 2, feats), bf16),
        pltpu.VMEM((keys // 2, feats), bf16),
        pltpu.VMEM((keys // 2, feats), bf16),
        pltpu.VMEM((keys // 2, feats), bf16),
        pltpu.VMEM((span, bw), f32),
        pltpu.VMEM((span, bw), f32),
        pltpu.VMEM((span, LANES), f32),
        pltpu.VMEM((groups, SUB, span), f32),
        [pltpu.VMEM((n, cuts, p, SUB, cut_cols), bf16) for p in parts],
        [pltpu.VMEM((n, cuts, p, SUB, cut_cols), bf16) for p in parts],
        [pltpu.VMEM((2, half + 1, cuts, p, SUB, cut_cols), bf16) for p in parts],
        [pltpu.VMEM((count, ff), bf16) for count in counts],
        [pltpu.VMEM((span, groups * size), bf16) for size in sizes],
        [pltpu.VMEM((span, groups * size), bf16) for size in sizes],
        [pltpu.VMEM((groups, p, SUB, bw), bf16) for p in parts[:-1]],
        [pltpu.VMEM((groups, p, SUB, bw), bf16) for p in parts[:-1]]
        + [pltpu.VMEM((groups, 3, parts[-1], SUB, bw), bf16)],
        dma((12,)),
        dma((len(parts),)),
        dma((len(parts), steps)),
        dma((len(parts),)),
        dma((len(parts), steps)),
        dma((4,)),
        dma((4,)),
        dma((len(parts),)),
        dma((len(parts),)),
        dma,
        dma,
        dma,
    ]
    teacher, student, loss = pl.pallas_call(
        functools.partial(layer_kernel, order, cap, parts, cuts),
        out_shape=(
            pltpu.VMEM((span, bw), bf16),
            pltpu.VMEM((span, bw), bf16),
            pltpu.VMEM((1, span), f32),
        ),
        in_specs=[hbm] * 12,
        out_specs=(vmem, vmem, vmem),
        scratch_shapes=scratch,
        compiler_params=pltpu.CompilerParams(
            collective_id=0, has_side_effects=True, vmem_limit_bytes=60 * 1024 * 1024
        ),
        name="layer",
    )(
        tokens,
        norm_gain.reshape(1, width),
        router_weight.T,
        expert_ids.T,
        gate_weight.reshape(width, ff),
        up_weight.reshape(width, ff),
        down_weight.reshape(ff, width),
        query_weight,
        key_weight,
        log_decay,
        carried_state.reshape(keys, feats),
        out_gain.reshape(1, bw),
    )
    teacher, student, loss = pl.pallas_call(
        result_kernel,
        out_shape=(
            jax.ShapeDtypeStruct((span, bw), bf16),
            jax.ShapeDtypeStruct((span, bw), bf16),
            jax.ShapeDtypeStruct((1, span), f32),
        ),
        in_specs=[vmem, vmem, vmem],
        out_specs=(hbm, hbm, hbm),
        scratch_shapes=[dma((3,))],
        name="result",
    )(*(pltpu.with_memory_space_constraint(x, pltpu.VMEM) for x in (teacher, student, loss)))
    return teacher, student, loss.reshape(span)


def solution(mesh):
    return jax.shard_map(
        functools.partial(on_device, tuple(ring_order(mesh))),
        mesh=mesh,
        in_specs=(
            P("seq", None),
            P(),
            P(),
            P("seq", None),
            P("expert", None, "seq"),
            P("expert", None, "seq"),
            P("expert", "seq", None),
            P(None, "expert"),
            P(None, "expert"),
            P("expert", "seq"),
            P("expert", None, None),
            P("expert"),
        ),
        out_specs=(P("seq", "expert"), P("seq", "expert"), P("seq")),
        check_vma=False,
    )
```
